128 devices in a mesh: col: 4 (over x), row: 32 (over z, y, core).
Axes of the slice: x: 4, y: 4, z: 4, core: 2. Of those that a mesh axis runs over, the one named last changes fastest.
Arguments:
- t_amps: float32 [1024, 20736], P('row', 'col')
- denoms: float32 [1024, 20736], P('row', 'col')
- v_oovv: bfloat16 [1024, 20736], P('row', 'col')
- v_vvvv: bfloat16 [20736, 20736], P('row', 'col')
- v_oooo: bfloat16 [1024, 1024], replicated
- w_direct: bfloat16 [4608, 4608], P(None, 'col')
- w_exch: bfloat16 [4608, 4608], P(None, 'col')
Outputs:
- output: float32 [1024, 20736], P('row', 'col')
All inputs are finite; a program needn't handle non-finite values.
Results may differ from the reference program's by a relative error of at most 0.001.
Values are sent between devices in bfloat16 or wider.
A program may use at most 1 GiB of HBM per device.

```python
import jax
import jax.numpy as jnp

OCC = 32
VIRT = 144
PAIRS_OCC = OCC * OCC
PAIRS_VIRT = VIRT * VIRT
PH_DIM = OCC * VIRT


def setup_inputs(seed: int = 0) -> dict:
    keys = jax.random.split(jax.random.key(seed), 7)
    amp_scale = 1.5 * (OCC * VIRT) ** -0.5
    t_amps = amp_scale * jax.random.normal(keys[0], (PAIRS_OCC, PAIRS_VIRT), jnp.float32)
    denoms = -jax.random.uniform(keys[1], (PAIRS_OCC, PAIRS_VIRT), jnp.float32, 1.0, 3.0)
    v_oovv = jax.random.normal(keys[2], (PAIRS_OCC, PAIRS_VIRT), jnp.float32).astype(jnp.bfloat16)
    vvvv_scale = (OCC / VIRT) ** 0.5 / 1.5
    v_vvvv = (vvvv_scale * jax.random.normal(keys[3], (PAIRS_VIRT, PAIRS_VIRT), jnp.float32)).astype(jnp.bfloat16)
    oooo_scale = (VIRT / OCC) ** 0.5 / 1.5
    v_oooo = (oooo_scale * jax.random.normal(keys[4], (PAIRS_OCC, PAIRS_OCC), jnp.float32)).astype(jnp.bfloat16)
    w_direct = (0.6 * jax.random.normal(keys[5], (PH_DIM, PH_DIM), jnp.float32)).astype(jnp.bfloat16)
    w_exch = (0.6 * jax.random.normal(keys[6], (PH_DIM, PH_DIM), jnp.float32)).astype(jnp.bfloat16)
    return {"t_amps": t_amps, "denoms": denoms, "v_oovv": v_oovv, "v_vvvv": v_vvvv, "v_oooo": v_oooo, "w_direct": w_direct, "w_exch": w_exch}


def reference(t_amps, denoms, v_oovv, v_vvvv, v_oooo, w_direct, w_exch):
    t_half = t_amps.astype(jnp.bfloat16)
    ladder = jnp.dot(t_half, v_vvvv, preferred_element_type=jnp.float32)
    inter_x = jnp.dot(v_oovv, t_half.T, preferred_element_type=jnp.float32)
    hole_mat = (v_oooo.astype(jnp.float32) + 0.5 * inter_x).astype(jnp.bfloat16)
    hole_term = jnp.dot(hole_mat.T, t_half, preferred_element_type=jnp.float32)
    t_wide = t_half.astype(jnp.float32).reshape(OCC, OCC, VIRT, VIRT)
    wd_wide = w_direct.astype(jnp.float32).reshape(OCC, VIRT, OCC, VIRT)
    wx_wide = w_exch.astype(jnp.float32).reshape(OCC, VIRT, OCC, VIRT)
    direct_term = jnp.einsum("ikac,kcjb->ijab", t_wide, wd_wide)
    exch_term = jnp.einsum("ikcb,kcja->ijab", t_wide, wx_wide)
    ph_net = direct_term - exch_term
    ph_sym = (ph_net + ph_net.transpose(1, 0, 3, 2)).reshape(PAIRS_OCC, PAIRS_VIRT)
    residual = v_oovv.astype(jnp.float32) + ladder + hole_term + ph_sym
    return residual / denoms
```

```python
import math
import jax
import jax.numpy as jnp
from jax import lax
from jax.sharding import PartitionSpec as P


def solution(mesh):
    n_row = mesh.shape["row"]
    n_col = mesh.shape["col"]
    amp_spec = P("row", "col")
    wide_spec = P(None, "col")

    def local_sweep(t_blk, d_blk, oovv_blk, vvvv_blk, oooo_full, wd_blk, wx_blk):
        f32 = jnp.float32
        rows_dev, cols_dev = t_blk.shape
        n_occ = math.isqrt(oooo_full.shape[0])
        n_virt = wd_blk.shape[0] // n_occ
        occ_col = n_occ // n_col
        virt_col = n_virt // n_col
        c_dev = vvvv_blk.shape[0]
        row_idx = lax.axis_index("row")
        t_half = t_blk.astype(jnp.bfloat16)
        t_rows = lax.all_gather(t_half, "col", axis=1, tiled=True)
        v_rows = lax.all_to_all(oovv_blk, "col", 0, 1, tiled=True)
        both = jnp.concatenate([t_rows, v_rows], axis=0)
        both = lax.all_to_all(both.reshape(rows_dev + occ_col, n_row, c_dev), "row", 1, 0, tiled=True)
        both = both.reshape(n_row, rows_dev + occ_col, c_dev)
        t_ladder = both[:, :rows_dev].reshape(n_row * rows_dev, c_dev)
        v_lad = both[:, rows_dev:].reshape(n_row * occ_col, c_dev)
        x_part = lax.dot_general(v_lad, t_ladder, (((1,), (1,)), ((), ())), preferred_element_type=f32)
        x_own = lax.psum_scatter(x_part, "row", scatter_dimension=0, tiled=True)
        start = row_idx * rows_dev + lax.axis_index("col") * occ_col
        oooo_rows = lax.dynamic_slice_in_dim(oooo_full, start, occ_col, axis=0)
        m_own = (oooo_rows.astype(f32) + 0.5 * x_own).astype(jnp.bfloat16)
        hole_mat = lax.all_gather(m_own, "col", axis=0, tiled=True)
        ladder_part = jnp.dot(t_ladder, vvvv_blk, preferred_element_type=f32)
        hole_part = lax.dot_general(hole_mat, t_half, (((0,), (0,)), ((), ())), preferred_element_type=f32)
        ladder_sum = lax.psum_scatter(ladder_part + hole_part, "row", scatter_dimension=0, tiled=True)

        t_four = t_rows.reshape(n_occ, n_virt, n_virt)
        lhs_d = t_four.transpose(1, 0, 2).reshape(n_virt, n_occ * n_virt)
        lhs_x = t_four.reshape(n_occ * n_virt, n_virt)
        out_d = jnp.dot(lhs_d, wd_blk, preferred_element_type=f32).reshape(n_virt, occ_col, n_virt)
        out_x = lax.dot_general(lhs_x, wx_blk, (((0,), (0,)), ((), ())), preferred_element_type=f32).reshape(n_virt, occ_col, n_virt)
        s_ab = out_d - out_x.transpose(2, 1, 0)
        s_ba = s_ab.transpose(2, 1, 0)
        pair = jnp.stack([s_ab.transpose(1, 0, 2), s_ba.transpose(1, 0, 2)])
        pair = pair.reshape(2, occ_col, n_col, virt_col * n_virt)
        pair = lax.all_to_all(pair, "col", 2, 1, tiled=True).reshape(2, n_occ, cols_dev)
        swapped = lax.all_to_all(pair[1], "row", 0, 0, tiled=True)
        ph_sym = pair[0] + swapped
        residual = oovv_blk.astype(f32) + ladder_sum + ph_sym
        return residual / d_blk

    return jax.shard_map(local_sweep, mesh=mesh, in_specs=(amp_spec, amp_spec, amp_spec, amp_spec, P(), wide_spec, wide_spec), out_specs=amp_spec, check_vma=False)
```

```python
import functools
import math
import jax
import jax.numpy as jnp
from jax import lax
from jax.experimental import pallas as pl
from jax.experimental.pallas import tpu as pltpu
from jax.sharding import PartitionSpec as P

MESH = pl.DeviceIdType.MESH
BF16 = jnp.bfloat16
F32 = jnp.float32
VMEM_LIMIT = 66 * 1000 * 1000


def _place():
    x = lax.axis_index("col")
    r = lax.axis_index("row")
    core = r % 2
    q = r // 2
    return x, q // 4, q % 4, core, q


def _rc(src, dst, ssem, rsem, dev):
    return pltpu.make_async_remote_copy(src_ref=src, dst_ref=dst, send_sem=ssem, recv_sem=rsem, device_id=dev, device_id_type=MESH)


def gather_kernel(ts, t2, vs, tl, vl, tr, g, g_s, g_r, t_s, t_r, p_s, p_r, v_s, v_r, f_s, f_r, loc):
    x, z, y, core, q = _place()
    r = lax.axis_index("row")
    right, left = (x + 1) % 4, (x + 3) % 4
    half = ts.shape[0] // 2
    hrow = t2.shape[0] // 2

    own = pltpu.make_async_copy(ts, g.at[x], loc.at[0])
    own.start()
    ag_r = _rc(ts, g.at[x], g_s.at[0], g_r.at[0], (right, r))
    ag_l = _rc(ts, g.at[x], g_s.at[1], g_r.at[1], (left, r))
    ag_r.start()
    ag_l.start()
    own2 = pltpu.make_async_copy(t2, tr.at[x], loc.at[2])
    own2.start()

    def v_copy(x2, yd):
        return _rc(vs.at[pl.ds(2 * yd, 2), x2], vl.at[:, core, q], v_s.at[x2, yd], v_r.at[q], (x2, (x * 4 + yd) * 2 + core))

    def v_each(fn_remote, fn_local):
        for i in range(4):
            for k in range(4):
                x2, yd = (x + i) % 4, (y + k) % 4
                if i == 0 and k == 0:
                    mine = x == z

                    @pl.when(mine)
                    def _():
                        fn_local(x2, yd)

                    @pl.when(jnp.logical_not(mine))
                    def _():
                        fn_remote(x2, yd)
                else:
                    fn_remote(x2, yd)

    own.wait()

    def t_copy(xs, yd):
        return _rc(g.at[xs, pl.ds(2 * yd, 2)], tl.at[:, q], t_s.at[xs, yd], t_r.at[q], (x, (xs * 4 + yd) * 2 + core))

    def t_block(rel):
        xs = (x + rel) % 4
        for k in range(4):
            yd = (y + k) % 4
            if k == 0:
                mine = xs == z

                @pl.when(mine)
                def _():
                    pltpu.make_async_copy(g.at[xs, pl.ds(2 * yd, 2)], tl.at[:, q], loc.at[1]).start()

                @pl.when(jnp.logical_not(mine))
                def _():
                    t_copy(xs, yd).start()
            else:
                t_copy(xs, yd).start()

    t_block(0)
    v_each(lambda a, b: v_copy(a, b).start(),
           lambda a, b: pltpu.make_async_copy(vs.at[pl.ds(2 * b, 2), a], vl.at[:, core, q], loc.at[3]).start())
    ag_r.wait_recv()
    fw_r = _rc(g.at[left, pl.ds(0, half)], g.at[left, pl.ds(0, half)], g_s.at[2], g_r.at[2], (right, r))
    fw_r.start()
    t_block(3)
    ag_l.wait_recv()
    fw_l = _rc(g.at[right, pl.ds(half, half)], g.at[right, pl.ds(half, half)], g_s.at[3], g_r.at[3], (left, r))
    fw_l.start()
    t_block(1)
    own2.wait()
    p_r0 = _rc(t2, tr.at[x], p_s.at[0], p_r.at[0], (right, r))
    p_l0 = _rc(t2, tr.at[x], p_s.at[1], p_r.at[1], (left, r))
    p_r0.start()
    p_l0.start()
    fw_r.wait_recv()
    fw_l.wait_recv()
    t_block(2)
    p_r0.wait_recv()
    pf_r = _rc(tr.at[left, pl.ds(0, hrow)], tr.at[left, pl.ds(0, hrow)], p_s.at[2], p_r.at[2], (right, r))
    pf_r.start()
    p_l0.wait_recv()
    pf_l = _rc(tr.at[right, pl.ds(hrow, hrow)], tr.at[right, pl.ds(hrow, hrow)], p_s.at[3], p_r.at[3], (left, r))
    pf_l.start()

    for k in range(16):
        qs = (q + k) % 16
        if k == 0:
            @pl.when(x == z)
            def _():
                pltpu.make_async_copy(vs.at[pl.ds(2 * y, 2), x], vl.at[:, core, q], loc.at[3]).wait()

            @pl.when(x != z)
            def _():
                _rc(vs.at[pl.ds(2 * y, 2), x], vl.at[:, core, qs], v_s.at[x, y], v_r.at[qs], (x, r)).wait_recv()
        else:
            _rc(vs.at[pl.ds(2 * y, 2), x], vl.at[:, core, qs], v_s.at[x, y], v_r.at[qs], (x, r)).wait_recv()
    fwd = _rc(vl.at[:, core], vl.at[:, core], f_s, f_r, (x, q * 2 + 1 - core))
    fwd.start()
    for k in range(16):
        qs = (q + k) % 16
        if k == 0:
            pltpu.make_async_copy(g.at[x, pl.ds(2 * y, 2)], tl.at[:, q], loc.at[1]).wait()
        else:
            _rc(g.at[x, pl.ds(2 * y, 2)], tl.at[:, qs], t_s.at[x, y], t_r.at[qs], (x, r)).wait_recv()
    fwd.wait()
    pf_r.wait_recv()
    pf_l.wait_recv()
    for c in (ag_r, ag_l, fw_r, fw_l, p_r0, p_l0, pf_r, pf_l):
        c.wait_send()
    for rel in range(4):
        xs = (x + rel) % 4
        for k in range(4):
            yd = (y + k) % 4
            if k == 0:
                @pl.when(xs != z)
                def _():
                    t_copy(xs, yd).wait_send()
            else:
                t_copy(xs, yd).wait_send()
    v_each(lambda a, b: v_copy(a, b).wait_send(), lambda a, b: None)


def gather_call(ts, t2, vs):
    n_p, rows, cw = ts.shape
    cols = t2.shape[1]
    dma = pltpu.SemaphoreType.DMA
    vm = pl.BlockSpec(memory_space=pltpu.VMEM)
    return pl.pallas_call(
        gather_kernel,
        out_shape=[
            jax.ShapeDtypeStruct((2, 16, rows, cw), BF16),
            jax.ShapeDtypeStruct((2, 2, 16, rows // 4, cw), BF16),
            jax.ShapeDtypeStruct((4, rows, cols), BF16),
        ],
        in_specs=[vm, vm, vm],
        out_specs=[vm, vm, vm],
        scratch_shapes=[
            pltpu.VMEM((4, n_p, rows, cw), BF16),
            dma((4,)), dma((4,)), dma((4, 4)), dma((16,)), dma((4,)), dma((4,)), dma((4, 4)), dma((16,)), dma, dma, dma((4,)),
        ],
        compiler_params=pltpu.CompilerParams(has_side_effects=True, vmem_limit_bytes=VMEM_LIMIT),
        name="gather",
    )(ts, t2, vs)


N_CH = 10
CW = 512
TAIL = 64


def ladder_kernel(tl, vl, v_hbm, t2, oo, out, v_buf, t_pair, m_t, x_part, x_in, m_all, p_b, p_t, r1, r1t, r2, r2t, qb, qt,
                  vl_s, vx_s, vx_r, tp_s, tp_r, x_s, x_r, m_s, m_r, s1, w1, s2, w2):
    x, z, y, core, q = _place()
    r = lax.axis_index("row")
    mate = (x, q * 2 + 1 - core)
    mcore = 1 - core
    n_c = v_hbm.shape[0]
    n_v = 9
    cols = [(i * 640, 640) for i in range(8)] + [(5120, 64)]

    v_in = []
    v_x = []
    for i, (c0, w) in enumerate(cols):
        a = pltpu.make_async_copy(v_hbm.at[:, pl.ds(c0, w)], v_buf.at[core, :, pl.ds(c0, w)], vl_s.at[i])
        b = _rc(v_hbm.at[:, pl.ds(c0, w)], v_buf.at[core, :, pl.ds(c0, w)], vx_s.at[i], vx_r.at[i], mate)
        a.start()
        b.start()
        v_in.append(a)
        v_x.append(b)
    tp_l = pltpu.make_async_copy(t2, t_pair.at[core], tp_s.at[0])
    tp_x = _rc(t2, t_pair.at[core], tp_s.at[1], tp_r, mate)
    tp_l.start()
    tp_x.start()

    rows = tl.shape[2]
    k8 = vl.shape[3]
    n_i = 16 * rows
    n_k = 32 * k8
    tl0 = tl[0].reshape(n_i, n_c)
    tl1 = tl[1].reshape(n_i, n_c)
    dn = (((1,), (1,)), ((), ()))
    xp = lax.dot_general(vl[0].reshape(n_k, n_c), tl0, dn, preferred_element_type=F32)
    xp = xp + lax.dot_general(vl[1].reshape(n_k, n_c), tl1, dn, preferred_element_type=F32)
    x_part[...] = xp.reshape(2, 16, k8, n_i)

    def x_copy(k):
        qd = (q + k) % 16
        return _rc(x_part.at[:, qd], x_in.at[q], x_s.at[k], x_r.at[k], (x, qd * 2 + core))

    for k in range(1, 16):
        x_copy(k).start()
    x_in[q] = x_part[:, q]
    for k in range(1, 16):
        x_copy(k).wait_recv()
    xs = x_in[0]
    for k in range(1, 16):
        xs = xs + x_in[k]
    m_all[x] = (oo[...].astype(F32) + 0.5 * xs).astype(BF16)

    def m_copy(k):
        return _rc(m_all.at[x], m_all.at[x], m_s.at[k], m_r.at[k], ((x + k) % 4, r))

    for k in range(1, 4):
        m_copy(k).start()
    tp_l.wait()
    tp_x.wait()
    for i in range(n_v):
        v_in[i].wait()
        v_x[i].wait()
    for k in range(1, 4):
        m_copy(k).wait_recv()
    mf = m_all[...].astype(F32)
    m_t[...] = jnp.concatenate([mf[xx, cc] for cc in range(2) for xx in range(4)], axis=0).T.astype(BF16)

    def coords(a):
        return y * a + z * (1 - a), z * a + y * (1 - a)

    def to1(a, d):
        yy = (y + d * a) % 4
        zz = (z + d * (1 - a)) % 4
        return (x, (zz * 4 + yy) * 2 + core)

    def to2(a, d):
        yy = (y + d * (1 - a)) % 4
        zz = (z + d * a) % 4
        return (x, (zz * 4 + yy) * 2 + core)

    def phase1(t, a, pb, rb):
        u, _ = coords(a)
        lo, hi = pl.ds(0, 2), pl.ds(2, 2)
        far, up, dn_ = (u + 2) % 4, (u + 1) % 4, (u + 3) % 4

        def mk(i, src, d):
            return _rc(pb.at[src], rb.at[i], s1.at[t, i], w1.at[t, i], to1(a, d))
        args = ((far, lo), 1), ((far, hi), 3), ((up, hi), 1), ((dn_, lo), 3), ((up, lo), 1), ((dn_, hi), 3)
        return lambda i: mk(i, *args[i])

    def phase2(t, a, pb, rb):
        u, v = coords(a)
        h = rows // 2
        lo, hi = pl.ds(0, h), pl.ds(h, h)
        far, up, dn_ = (v + 2) % 4, (v + 1) % 4, (v + 3) % 4

        def mk(i, src, d):
            return _rc(pb.at[src], rb.at[i], s2.at[t, i], w2.at[t, i], to2(a, d))
        args = ((u, far, lo), 1), ((u, far, hi), 3), ((u, up, hi), 1), ((u, dn_, lo), 3), ((u, up, lo), 1), ((u, dn_, hi), 3)
        return lambda i: mk(i, *args[i])

    def bufs(t):
        return p_b.at[t], r1.at[t], r2.at[t]

    def compute(t, a, pb, c0, w):
        vb0 = v_buf[0, :, pl.ds(c0, w)]
        vb1 = v_buf[1, :, pl.ds(c0, w)]
        tp = t_pair[:, :, pl.ds(c0, w)].reshape(2 * rows, w)
        acc = jnp.dot(tl[0].reshape(n_i, n_c), vb0, preferred_element_type=F32)
        acc = acc + jnp.dot(tl[1].reshape(n_i, n_c), vb1, preferred_element_type=F32)
        acc = acc + jnp.dot(m_t[...], tp, preferred_element_type=F32)
        for zb in range(4):
            for yb in range(4):
                b = zb * 4 + yb
                pb[yb * a + zb * (1 - a), zb * a + yb * (1 - a)] = acc[b * rows:(b + 1) * rows]

    def l1(t, a, pb, rb, c0, w):
        compute(t, a, pb, c0, w)
        cs = phase1(t, a, pb, rb)
        for i in range(4):
            cs(i).start()

    def l2(t, a, pb, rb):
        u, _ = coords(a)
        cs = phase1(t, a, pb, rb)
        up, dn_ = (u + 1) % 4, (u + 3) % 4
        cs(0).wait_recv()
        pb[up, 0:2] = pb[up, 0:2] + rb[0]
        cs(4).start()
        cs(1).wait_recv()
        pb[dn_, 2:4] = pb[dn_, 2:4] + rb[1]
        cs(5).start()

    def l3(t, a, pb, rb, rb2):
        u, _ = coords(a)
        cs = phase1(t, a, pb, rb)
        for i in (3, 2, 4, 5):
            cs(i).wait_recv()
        pb[u, 0:2] = pb[u, 0:2] + rb[4] + rb[3]
        pb[u, 2:4] = pb[u, 2:4] + rb[2] + rb[5]
        cs = phase2(t, a, pb, rb2)
        for i in range(4):
            cs(i).start()

    def l4(t, a, pb, rb2):
        u, v = coords(a)
        h = rows // 2
        cs = phase2(t, a, pb, rb2)
        up, dn_ = (v + 1) % 4, (v + 3) % 4
        cs(0).wait_recv()
        pb[u, up, 0:h] = pb[u, up, 0:h] + rb2[0]
        cs(4).start()
        cs(1).wait_recv()
        pb[u, dn_, h:rows] = pb[u, dn_, h:rows] + rb2[1]
        cs(5).start()

    def l5(t, a, pb, rb, rb2, c0, w):
        u, v = coords(a)
        h = rows // 2
        cs = phase2(t, a, pb, rb2)
        for i in (2, 3, 4, 5):
            cs(i).wait_recv()
        out[0:h, pl.ds(c0, w)] = pb[u, v, 0:h] + rb2[4] + rb2[3]
        out[h:rows, pl.ds(c0, w)] = pb[u, v, h:rows] + rb2[2] + rb2[5]
        ds = phase1(t, a, pb, rb)
        for i in range(6):
            cs(i).wait_send()
            ds(i).wait_send()

    def kind(t):
        return 1 - t % 2

    def col0(t):
        return pl.multiple_of((t // 2) * CW + (t % 2) * (N_CH // 2) * CW, 128)

    ct = N_CH * CW
    l1(N_CH, 1, p_t, r1t, ct, TAIL)

    def f1(t, c):
        pb, rb, _ = bufs(t)
        l1(t, kind(t), pb, rb, col0(t), CW)
        return c
    lax.fori_loop(0, N_CH, f1, 0)
    l2(N_CH, 1, p_t, r1t)

    def f2(t, c):
        pb, rb, _ = bufs(t)
        l2(t, kind(t), pb, rb)
        return c
    lax.fori_loop(0, N_CH, f2, 0)
    l3(N_CH, 1, p_t, r1t, r2t)
    l4(N_CH, 1, p_t, r2t)
    pb, rb, rb2 = bufs(0)
    l3(0, 1, pb, rb, rb2)

    def f3(t, c):
        pb, rb, rb2 = bufs(t)
        l3(t, kind(t), pb, rb, rb2)
        pb, rb, rb2 = bufs(t - 1)
        l4(t - 1, kind(t - 1), pb, rb2)
        return c
    lax.fori_loop(1, N_CH, f3, 0)
    pb, rb, rb2 = bufs(N_CH - 1)
    l4(N_CH - 1, (N_CH % 2), pb, rb2)
    l5(N_CH, 1, p_t, r1t, r2t, ct, TAIL)

    def f5(t, c):
        pb, rb, rb2 = bufs(t)
        l5(t, kind(t), pb, rb, rb2, col0(t), CW)
        return c
    lax.fori_loop(0, N_CH, f5, 0)
    for k in range(1, 16):
        x_copy(k).wait_send()
    for k in range(1, 4):
        m_copy(k).wait_send()


def ladder_call(tl, vl, v, t2, oo):
    _, _, rows, n_c = tl.shape
    k8 = vl.shape[3]
    cols = t2.shape[1]
    dma = pltpu.SemaphoreType.DMA
    vm = pl.BlockSpec(memory_space=pltpu.VMEM)
    n = N_CH + 1
    return pl.pallas_call(
        ladder_kernel,
        out_shape=jax.ShapeDtypeStruct((rows, cols), F32),
        in_specs=[vm, vm, pl.BlockSpec(memory_space=pl.ANY), vm, vm],
        out_specs=vm,
        scratch_shapes=[
            pltpu.VMEM((2, n_c, cols), BF16),
            pltpu.VMEM((2, rows, cols), BF16),
            pltpu.VMEM((16 * rows, 8 * k8), BF16),
            pltpu.VMEM((2, 16, k8, 16 * rows), F32),
            pltpu.VMEM((16, 2, k8, 16 * rows), F32),
            pltpu.VMEM((4, 2, k8, 16 * rows), BF16),
            pltpu.VMEM((N_CH, 4, 4, rows, CW), F32),
            pltpu.VMEM((4, 4, rows, TAIL), F32),
            pltpu.VMEM((N_CH, 6, 2, rows, CW), F32),
            pltpu.VMEM((6, 2, rows, TAIL), F32),
            pltpu.VMEM((N_CH, 6, rows // 2, CW), F32),
            pltpu.VMEM((6, rows // 2, TAIL), F32),
            pltpu.VMEM((8, 128), F32),
            pltpu.VMEM((8, 128), F32),
            dma((9,)), dma((9,)), dma((9,)), dma((2,)), dma, dma((16,)), dma((16,)), dma((4,)), dma((4,)),
            dma((n, 6)), dma((n, 6)), dma((n, 6)), dma((n, 6)),
        ],
        compiler_params=pltpu.CompilerParams(has_side_effects=True, vmem_limit_bytes=VMEM_LIMIT),
        name="ladder",
    )(tl, vl, v, t2, oo)


def solution(mesh):
    n_row = mesh.shape["row"]
    n_col = mesh.shape["col"]
    amp_spec = P("row", "col")
    wide_spec = P(None, "col")

    def local_sweep(t_blk, d_blk, oovv_blk, vvvv_blk, oooo_full, wd_blk, wx_blk):
        rows_dev, cols_dev = t_blk.shape
        n_occ = math.isqrt(oooo_full.shape[0])
        n_virt = wd_blk.shape[0] // n_occ
        occ_col = n_occ // n_col
        virt_col = n_virt // n_col
        c_dev = vvvv_blk.shape[0]
        n_p = cols_dev // c_dev
        q = lax.axis_index("row") // 2
        core = lax.axis_index("row") % 2
        t_half = t_blk.astype(BF16)
        ts = t_half.reshape(rows_dev, n_p, c_dev).transpose(1, 0, 2)
        vs = oovv_blk.reshape(n_col, occ_col, n_p, c_dev).transpose(2, 0, 1, 3)
        tl, vl, tr = gather_call(ts, t_half, vs)
        oo = oooo_full.reshape(16, 2, n_col, occ_col, 16, 2, n_occ)
        oo = lax.dynamic_index_in_dim(oo, q, 0, False)
        oo = lax.dynamic_index_in_dim(oo, lax.axis_index("col"), 1, False)
        oo = lax.dynamic_index_in_dim(oo, core, 3, False)
        oo = oo.reshape(2, occ_col, 16 * n_occ)
        ladder_sum = ladder_call(tl, vl, vvvv_blk, t_half, oo)

        t_four = tr.reshape(n_col, n_occ, virt_col, n_virt).transpose(1, 0, 2, 3).reshape(n_occ, n_virt, n_virt)
        lhs_d = t_four.transpose(1, 0, 2).reshape(n_virt, n_occ * n_virt)
        lhs_x = t_four.reshape(n_occ * n_virt, n_virt)
        out_d = jnp.dot(lhs_d, wd_blk, preferred_element_type=F32).reshape(n_virt, occ_col, n_virt)
        out_x = lax.dot_general(lhs_x, wx_blk, (((0,), (0,)), ((), ())), preferred_element_type=F32).reshape(n_virt, occ_col, n_virt)
        s_ab = out_d - out_x.transpose(2, 1, 0)
        s_ba = s_ab.transpose(2, 1, 0)
        pair = jnp.stack([s_ab.transpose(1, 0, 2), s_ba.transpose(1, 0, 2)])
        pair = pair.reshape(2, occ_col, n_col, virt_col * n_virt)
        pair = lax.all_to_all(pair, "col", 2, 1, tiled=True).reshape(2, n_occ, cols_dev)
        swapped = lax.all_to_all(pair[1], "row", 0, 0, tiled=True)
        ph_sym = pair[0] + swapped
        residual = oovv_blk.astype(F32) + ladder_sum + ph_sym
        return residual / d_blk

    return jax.shard_map(local_sweep, mesh=mesh, in_specs=(amp_spec, amp_spec, amp_spec, amp_spec, P(), wide_spec, wide_spec), out_specs=amp_spec, check_vma=False)
```

```python
import functools
import math
import jax
import jax.numpy as jnp
from jax import lax
from jax.experimental import pallas as pl
from jax.experimental.pallas import tpu as pltpu
from jax.sharding import PartitionSpec as P

MESH = pl.DeviceIdType.MESH
BF16 = jnp.bfloat16
F32 = jnp.float32
VMEM_LIMIT = 66 * 1000 * 1000


def _place():
    x = lax.axis_index("col")
    r = lax.axis_index("row")
    core = r % 2
    q = r // 2
    return x, q // 4, q % 4, core, q


def _rc(src, dst, ssem, rsem, dev):
    return pltpu.make_async_remote_copy(src_ref=src, dst_ref=dst, send_sem=ssem, recv_sem=rsem, device_id=dev, device_id_type=MESH)


def gather_kernel(ts, l1, l2, vs, wd, wx, tl, vl, w, g, lg1, lg2, wdb, wxb, wxs, d_n, e_n, w1_n, w2_n, g_s, g_r, t_s, t_r, p_s, p_r, o_s, o_r, v_s, v_r, f_s, f_r, loc, w_s):
    x, z, y, core, q = _place()
    r = lax.axis_index("row")
    right, left = (x + 1) % 4, (x + 3) % 4
    half = ts.shape[0] // 2

    own = pltpu.make_async_copy(ts, g.at[x], loc.at[0])
    own.start()
    ag_r = _rc(ts, g.at[x], g_s.at[0], g_r.at[0], (right, r))
    ag_l = _rc(ts, g.at[x], g_s.at[1], g_r.at[1], (left, r))
    ag_r.start()
    ag_l.start()
    own1 = pltpu.make_async_copy(l1, lg1.at[x], loc.at[2])
    own2 = pltpu.make_async_copy(l2, lg2.at[x], loc.at[4])
    own1.start()
    own2.start()
    w_in = []
    for i in range(4):
        w_in.append(pltpu.make_async_copy(wd.at[pl.ds(8 * i, 8)], wdb.at[i], w_s.at[i]))
    for i in range(4):
        w_in.append(pltpu.make_async_copy(wx.at[:, pl.ds(32 * i + 8 * ((i + 1) // 2), 32)], wxb.at[i], w_s.at[4 + i]))
    for i in range(2):
        w_in.append(pltpu.make_async_copy(wx.at[:, pl.ds(32 + 72 * i, 8)], wxs.at[i], w_s.at[8 + i]))
    for c in w_in:
        c.start()

    def v_copy(x2, yd):
        return _rc(vs.at[pl.ds(2 * yd, 2), x2], vl.at[:, core, q], v_s.at[x2, yd], v_r.at[q], (x2, (x * 4 + yd) * 2 + core))

    def v_each(fn_remote, fn_local):
        for i in range(4):
            for k in range(4):
                x2, yd = (x + i) % 4, (y + k) % 4
                if i == 0 and k == 0:
                    mine = x == z

                    @pl.when(mine)
                    def _():
                        fn_local(x2, yd)

                    @pl.when(jnp.logical_not(mine))
                    def _():
                        fn_remote(x2, yd)
                else:
                    fn_remote(x2, yd)

    own.wait()

    def t_copy(xs, yd):
        return _rc(g.at[xs, pl.ds(2 * yd, 2)], tl.at[:, q], t_s.at[xs, yd], t_r.at[q], (x, (xs * 4 + yd) * 2 + core))

    def t_block(rel):
        xs = (x + rel) % 4
        for k in range(4):
            yd = (y + k) % 4
            if k == 0:
                mine = xs == z

                @pl.when(mine)
                def _():
                    pltpu.make_async_copy(g.at[xs, pl.ds(2 * yd, 2)], tl.at[:, q], loc.at[1]).start()

                @pl.when(jnp.logical_not(mine))
                def _():
                    t_copy(xs, yd).start()
            else:
                t_copy(xs, yd).start()

    t_block(0)
    v_each(lambda a, b: v_copy(a, b).start(),
           lambda a, b: pltpu.make_async_copy(vs.at[pl.ds(2 * b, 2), a], vl.at[:, core, q], loc.at[3]).start())
    ag_r.wait_recv()
    fw_r = _rc(g.at[left, pl.ds(0, half)], g.at[left, pl.ds(0, half)], g_s.at[2], g_r.at[2], (right, r))
    fw_r.start()
    t_block(3)
    ag_l.wait_recv()
    fw_l = _rc(g.at[right, pl.ds(half, half)], g.at[right, pl.ds(half, half)], g_s.at[3], g_r.at[3], (left, r))
    fw_l.start()
    t_block(1)
    def ring(src, buf, ss, rr, h, ax):
        def part(i):
            return (pl.ds(i * h, h),) if ax == 0 else (slice(None), pl.ds(i * h, h))
        return (_rc(src, buf.at[x], ss.at[0], rr.at[0], (right, r)), _rc(src, buf.at[x], ss.at[1], rr.at[1], (left, r)),
                lambda: _rc(buf.at[(left,) + part(0)], buf.at[(left,) + part(0)], ss.at[2], rr.at[2], (right, r)),
                lambda: _rc(buf.at[(right,) + part(1)], buf.at[(right,) + part(1)], ss.at[3], rr.at[3], (left, r)))

    a0, a1, a2, a3 = ring(l1, lg1, p_s, p_r, l1.shape[1] // 2, 1)
    a0.start()
    a1.start()
    b0, b1, b2, b3 = ring(l2, lg2, o_s, o_r, l2.shape[1] // 2, 1)
    b0.start()
    b1.start()
    fw_r.wait_recv()
    fw_l.wait_recv()
    t_block(2)
    a0.wait_recv()
    a2 = a2()
    a2.start()
    a1.wait_recv()
    a3 = a3()
    a3.start()
    b0.wait_recv()
    b2 = b2()
    b2.start()
    b1.wait_recv()
    b3 = b3()
    b3.start()

    def r3_r5():
        n1, kk = l1.shape
        nj = wd.shape[2]
        nb = l2.shape[0]
        nv = wd.shape[1]
        own1.wait()
        own2.wait()
        a2.wait_recv()
        a3.wait_recv()
        acc = None
        for i in range(4):
            w_in[i].wait()
            lhs = lg1[:, :, i * 8 * nv:(i + 1) * 8 * nv].reshape(4 * n1, 8 * nv)
            d = jnp.dot(lhs, wdb[i].reshape(8 * nv, nj), preferred_element_type=F32)
            acc = d if acc is None else acc + d
        for i in range(4):
            d_n[nv // 4 * i:nv // 4 * (i + 1), :] = acc[n1 * i:n1 * i + nv // 4]
        b2.wait_recv()
        b3.wait_recv()
        acc = None
        kb = 1024
        for i in range(4):
            w_in[4 + i].wait()
            d = jnp.dot(lg2[i, :, 0:kb], wxb[i].reshape(kb, nj), preferred_element_type=F32)
            acc = d if acc is None else acc + d
        for i in range(2):
            w_in[8 + i].wait()
            lhs = lg2[2 * i, :, kb:] + lg2[2 * i + 1, :, kb:]
            acc = acc + jnp.dot(lhs, wxs[i].reshape(256, nj), preferred_element_type=F32)
        e_n[...] = acc
        for j in range(nj // nv):
            w1 = d_n[:, j * nv:(j + 1) * nv] - e_n[:, j * nv:(j + 1) * nv].T
            w1_n[:, j * nv:(j + 1) * nv] = w1
            w2_n[:, j * nv:(j + 1) * nv] = w1.T
        for i in range(4):
            w[0, i, 0:nv // 4, :] = w1_n[nv // 4 * i:nv // 4 * (i + 1), :]
            w[1, i, 0:nv // 4, :] = w2_n[nv // 4 * i:nv // 4 * (i + 1), :]

    r3_r5()

    for k in range(16):
        qs = (q + k) % 16
        if k == 0:
            @pl.when(x == z)
            def _():
                pltpu.make_async_copy(vs.at[pl.ds(2 * y, 2), x], vl.at[:, core, q], loc.at[3]).wait()

            @pl.when(x != z)
            def _():
                _rc(vs.at[pl.ds(2 * y, 2), x], vl.at[:, core, qs], v_s.at[x, y], v_r.at[qs], (x, r)).wait_recv()
        else:
            _rc(vs.at[pl.ds(2 * y, 2), x], vl.at[:, core, qs], v_s.at[x, y], v_r.at[qs], (x, r)).wait_recv()
    fwd = _rc(vl.at[:, core], vl.at[:, core], f_s, f_r, (x, q * 2 + 1 - core))
    fwd.start()
    for k in range(16):
        qs = (q + k) % 16
        if k == 0:
            pltpu.make_async_copy(g.at[x, pl.ds(2 * y, 2)], tl.at[:, q], loc.at[1]).wait()
        else:
            _rc(g.at[x, pl.ds(2 * y, 2)], tl.at[:, qs], t_s.at[x, y], t_r.at[qs], (x, r)).wait_recv()
    fwd.wait()
    for c in (ag_r, ag_l, fw_r, fw_l, a0, a1, a2, a3, b0, b1, b2, b3):
        c.wait_send()
    for rel in range(4):
        xs = (x + rel) % 4
        for k in range(4):
            yd = (y + k) % 4
            if k == 0:
                @pl.when(xs != z)
                def _():
                    t_copy(xs, yd).wait_send()
            else:
                t_copy(xs, yd).wait_send()
    v_each(lambda a, b: v_copy(a, b).wait_send(), lambda a, b: None)


def gather_call(ts, l1, l2, vs, wd, wx):
    n_p, rows, cw = ts.shape
    dma = pltpu.SemaphoreType.DMA
    vm = pl.BlockSpec(memory_space=pltpu.VMEM)
    hbm = pl.BlockSpec(memory_space=pl.ANY)
    n_k, n_v, n_j = wd.shape
    return pl.pallas_call(
        gather_kernel,
        out_shape=[
            jax.ShapeDtypeStruct((2, 16, rows, cw), BF16),
            jax.ShapeDtypeStruct((2, 2, 16, rows // 4, cw), BF16),
            jax.ShapeDtypeStruct((2, 4, n_v // 4 + 4, n_j), F32),
        ],
        in_specs=[vm, vm, vm, vm, hbm, hbm],
        out_specs=[vm, vm, vm],
        scratch_shapes=[
            pltpu.VMEM((4, n_p, rows, cw), BF16),
            pltpu.VMEM((4,) + l1.shape, BF16),
            pltpu.VMEM((4,) + l2.shape, BF16),
            pltpu.VMEM((4, 8, n_v, n_j), BF16),
            pltpu.VMEM((4, n_k, 32, n_j), BF16),
            pltpu.VMEM((2, n_k, 8, n_j), BF16),
            pltpu.VMEM((n_v, n_j), F32),
            pltpu.VMEM((n_v, n_j), F32),
            pltpu.VMEM((n_v, n_j), F32),
            pltpu.VMEM((n_v, n_j), F32),
            dma((4,)), dma((4,)), dma((4, 4)), dma((16,)), dma((4,)), dma((4,)), dma((4,)), dma((4,)), dma((4, 4)), dma((16,)), dma, dma,
            dma((5,)), dma((10,)),
        ],
        compiler_params=pltpu.CompilerParams(has_side_effects=True, vmem_limit_bytes=VMEM_LIMIT),
        name="gather",
    )(ts, l1, l2, vs, wd, wx)


N_CH = 10
CW = 512
TAIL = 64


def ladder_kernel(tl, vl, v_hbm, t2, oo, sw, out, s1_in, ps_in, s2_in, v_buf, t_pair, m_t, x_part, x_in, m_all, p_b, p_t, r1, r1t, r2, r2t, qb, qt,
                  vl_s, vx_s, vx_r, tp_s, tp_r, x_s, x_r, m_s, m_r, s1, w1, s2, w2, sw_s, sw_r, ps_s, ps_r, sl):
    x, z, y, core, q = _place()
    r = lax.axis_index("row")
    mate = (x, q * 2 + 1 - core)
    mcore = 1 - core
    n_c = v_hbm.shape[0]
    n_v = 9
    cols = [(i * 640, 640) for i in range(8)] + [(5120, 64)]

    def s_copy(i, k):
        xd = (x + k) % 4
        return _rc(sw.at[i, xd], (s1_in, s2_in)[i].at[x], sw_s.at[i, k], sw_r.at[i, k], (xd, r))

    s_own = [pltpu.make_async_copy(sw.at[i, x], (s1_in, s2_in)[i].at[x], sl.at[i]) for i in range(2)]
    for i in (1, 0):
        for k in range(1, 4):
            s_copy(i, k).start()
        s_own[i].start()

    def ps_src(rd):
        j = rd % 8
        return s2_in.at[rd // 8, :, pl.ds(pl.multiple_of(9 * j // 8 * 128, 128), 256)]

    def ps_copy(k):
        rd = (r + k) % 32
        return _rc(ps_src(rd), ps_in.at[r], ps_s.at[k], ps_r.at[k], (x, rd))

    ps_own = pltpu.make_async_copy(ps_src(r), ps_in.at[r], sl.at[2])

    def ps_send():
        s_own[1].wait()
        for k in range(1, 4):
            s_copy(1, k).wait_recv()
        ps_own.start()
        for k in range(1, 32):
            ps_copy(k).start()

    v_in = []
    v_x = []
    for i, (c0, w) in enumerate(cols):
        a = pltpu.make_async_copy(v_hbm.at[:, pl.ds(c0, w)], v_buf.at[core, :, pl.ds(c0, w)], vl_s.at[i])
        b = _rc(v_hbm.at[:, pl.ds(c0, w)], v_buf.at[core, :, pl.ds(c0, w)], vx_s.at[i], vx_r.at[i], mate)
        a.start()
        b.start()
        v_in.append(a)
        v_x.append(b)
    tp_l = pltpu.make_async_copy(t2, t_pair.at[core], tp_s.at[0])
    tp_x = _rc(t2, t_pair.at[core], tp_s.at[1], tp_r, mate)
    tp_l.start()
    tp_x.start()

    rows = tl.shape[2]
    k8 = vl.shape[3]
    n_i = 16 * rows
    n_k = 32 * k8
    tl0 = tl[0].reshape(n_i, n_c)
    tl1 = tl[1].reshape(n_i, n_c)
    dn = (((1,), (1,)), ((), ()))
    xp = lax.dot_general(vl[0].reshape(n_k, n_c), tl0, dn, preferred_element_type=F32)
    xp = xp + lax.dot_general(vl[1].reshape(n_k, n_c), tl1, dn, preferred_element_type=F32)
    x_part[...] = xp.reshape(2, 16, k8, n_i)

    def x_copy(k):
        qd = (q + k) % 16
        return _rc(x_part.at[:, qd], x_in.at[q], x_s.at[k], x_r.at[k], (x, qd * 2 + core))

    for k in range(1, 16):
        x_copy(k).start()
    x_in[q] = x_part[:, q]
    for k in range(1, 16):
        x_copy(k).wait_recv()
    xs = x_in[0]
    for k in range(1, 16):
        xs = xs + x_in[k]
    m_all[x] = (oo[...].astype(F32) + 0.5 * xs).astype(BF16)

    def m_copy(k):
        return _rc(m_all.at[x], m_all.at[x], m_s.at[k], m_r.at[k], ((x + k) % 4, r))

    for k in range(1, 4):
        m_copy(k).start()
    tp_l.wait()
    tp_x.wait()
    for i in range(n_v):
        v_in[i].wait()
        v_x[i].wait()
    for k in range(1, 4):
        m_copy(k).wait_recv()
    mf = m_all[...].astype(F32)
    m_t[...] = jnp.concatenate([mf[xx, cc] for cc in range(2) for xx in range(4)], axis=0).T.astype(BF16)

    def coords(a):
        return y * a + z * (1 - a), z * a + y * (1 - a)

    def to1(a, d):
        yy = (y + d * a) % 4
        zz = (z + d * (1 - a)) % 4
        return (x, (zz * 4 + yy) * 2 + core)

    def to2(a, d):
        yy = (y + d * (1 - a)) % 4
        zz = (z + d * a) % 4
        return (x, (zz * 4 + yy) * 2 + core)

    def phase1(t, a, pb, rb):
        u, _ = coords(a)
        lo, hi = pl.ds(0, 2), pl.ds(2, 2)
        far, up, dn_ = (u + 2) % 4, (u + 1) % 4, (u + 3) % 4

        def mk(i, src, d):
            return _rc(pb.at[src], rb.at[i], s1.at[t, i], w1.at[t, i], to1(a, d))
        args = ((far, lo), 1), ((far, hi), 3), ((up, hi), 1), ((dn_, lo), 3), ((up, lo), 1), ((dn_, hi), 3)
        return lambda i: mk(i, *args[i])

    def phase2(t, a, pb, rb):
        u, v = coords(a)
        h = rows // 2
        lo, hi = pl.ds(0, h), pl.ds(h, h)
        far, up, dn_ = (v + 2) % 4, (v + 1) % 4, (v + 3) % 4

        def mk(i, src, d):
            return _rc(pb.at[src], rb.at[i], s2.at[t, i], w2.at[t, i], to2(a, d))
        args = ((u, far, lo), 1), ((u, far, hi), 3), ((u, up, hi), 1), ((u, dn_, lo), 3), ((u, up, lo), 1), ((u, dn_, hi), 3)
        return lambda i: mk(i, *args[i])

    def bufs(t):
        return p_b.at[t], r1.at[t], r2.at[t]

    def compute(t, a, pb, c0, w):
        vb0 = v_buf[0, :, pl.ds(c0, w)]
        vb1 = v_buf[1, :, pl.ds(c0, w)]
        tp = t_pair[:, :, pl.ds(c0, w)].reshape(2 * rows, w)
        acc = jnp.dot(tl[0].reshape(n_i, n_c), vb0, preferred_element_type=F32)
        acc = acc + jnp.dot(tl[1].reshape(n_i, n_c), vb1, preferred_element_type=F32)
        acc = acc + jnp.dot(m_t[...], tp, preferred_element_type=F32)
        for zb in range(4):
            for yb in range(4):
                b = zb * 4 + yb
                pb[yb * a + zb * (1 - a), zb * a + yb * (1 - a)] = acc[b * rows:(b + 1) * rows]

    def l1(t, a, pb, rb, c0, w):
        compute(t, a, pb, c0, w)
        cs = phase1(t, a, pb, rb)
        for i in range(4):
            cs(i).start()

    def l2(t, a, pb, rb):
        u, _ = coords(a)
        cs = phase1(t, a, pb, rb)
        up, dn_ = (u + 1) % 4, (u + 3) % 4
        cs(0).wait_recv()
        pb[up, 0:2] = pb[up, 0:2] + rb[0]
        cs(4).start()
        cs(1).wait_recv()
        pb[dn_, 2:4] = pb[dn_, 2:4] + rb[1]
        cs(5).start()

    def l3(t, a, pb, rb, rb2):
        u, _ = coords(a)
        cs = phase1(t, a, pb, rb)
        for i in (3, 2, 4, 5):
            cs(i).wait_recv()
        pb[u, 0:2] = pb[u, 0:2] + rb[4] + rb[3]
        pb[u, 2:4] = pb[u, 2:4] + rb[2] + rb[5]
        cs = phase2(t, a, pb, rb2)
        for i in range(4):
            cs(i).start()

    def l4(t, a, pb, rb2):
        u, v = coords(a)
        h = rows // 2
        cs = phase2(t, a, pb, rb2)
        up, dn_ = (v + 1) % 4, (v + 3) % 4
        cs(0).wait_recv()
        pb[u, up, 0:h] = pb[u, up, 0:h] + rb2[0]
        cs(4).start()
        cs(1).wait_recv()
        pb[u, dn_, h:rows] = pb[u, dn_, h:rows] + rb2[1]
        cs(5).start()

    def l5(t, a, pb, rb, rb2, c0, w):
        u, v = coords(a)
        h = rows // 2
        cs = phase2(t, a, pb, rb2)
        for i in (2, 3, 4, 5):
            cs(i).wait_recv()
        out[0:h, pl.ds(c0, w)] = pb[u, v, 0:h] + rb2[4] + rb2[3]
        out[h:rows, pl.ds(c0, w)] = pb[u, v, h:rows] + rb2[2] + rb2[5]
        ds = phase1(t, a, pb, rb)
        for i in range(6):
            cs(i).wait_send()
            ds(i).wait_send()

    def kind(t):
        return 1 - t % 2

    def col0(t):
        return pl.multiple_of((t // 2) * CW + (t % 2) * (N_CH // 2) * CW, 128)

    ct = N_CH * CW
    l1(N_CH, 1, p_t, r1t, ct, TAIL)

    def f1(t, c):
        pb, rb, _ = bufs(t)
        l1(t, kind(t), pb, rb, col0(t), CW)
        return c
    lax.fori_loop(0, N_CH, f1, 0)
    ps_send()
    l2(N_CH, 1, p_t, r1t)

    def f2(t, c):
        pb, rb, _ = bufs(t)
        l2(t, kind(t), pb, rb)
        return c
    lax.fori_loop(0, N_CH, f2, 0)
    l3(N_CH, 1, p_t, r1t, r2t)
    l4(N_CH, 1, p_t, r2t)
    pb, rb, rb2 = bufs(0)
    l3(0, 1, pb, rb, rb2)

    def f3(t, c):
        pb, rb, rb2 = bufs(t)
        l3(t, kind(t), pb, rb, rb2)
        pb, rb, rb2 = bufs(t - 1)
        l4(t - 1, kind(t - 1), pb, rb2)
        return c
    lax.fori_loop(1, N_CH, f3, 0)
    pb, rb, rb2 = bufs(N_CH - 1)
    l4(N_CH - 1, (N_CH % 2), pb, rb2)
    l5(N_CH, 1, p_t, r1t, r2t, ct, TAIL)

    def f5(t, c):
        pb, rb, rb2 = bufs(t)
        l5(t, kind(t), pb, rb, rb2, col0(t), CW)
        return c
    lax.fori_loop(0, N_CH, f5, 0)
    for k in range(1, 16):
        x_copy(k).wait_send()
    for k in range(1, 4):
        m_copy(k).wait_send()
    s_own[0].wait()
    ps_own.wait()
    for k in range(1, 32):
        ps_copy(k).wait()
    for k in range(1, 4):
        s_copy(0, k).wait()
        s_copy(1, k).wait_send()


def ladder_call(tl, vl, v, t2, oo, sw):
    _, _, rows, n_c = tl.shape
    k8 = vl.shape[3]
    cols = t2.shape[1]
    dma = pltpu.SemaphoreType.DMA
    vm = pl.BlockSpec(memory_space=pltpu.VMEM)
    n = N_CH + 1
    return pl.pallas_call(
        ladder_kernel,
        out_shape=[
            jax.ShapeDtypeStruct((rows, cols), F32),
            jax.ShapeDtypeStruct(sw.shape[1:], F32),
            jax.ShapeDtypeStruct((32, sw.shape[2], 256), F32),
        ],
        in_specs=[vm, vm, pl.BlockSpec(memory_space=pl.ANY), vm, vm, vm],
        out_specs=[vm, vm, vm],
        scratch_shapes=[
            pltpu.VMEM(sw.shape[1:], F32),
            pltpu.VMEM((2, n_c, cols), BF16),
            pltpu.VMEM((2, rows, cols), BF16),
            pltpu.VMEM((16 * rows, 8 * k8), BF16),
            pltpu.VMEM((2, 16, k8, 16 * rows), F32),
            pltpu.VMEM((16, 2, k8, 16 * rows), F32),
            pltpu.VMEM((4, 2, k8, 16 * rows), BF16),
            pltpu.VMEM((N_CH, 4, 4, rows, CW), F32),
            pltpu.VMEM((4, 4, rows, TAIL), F32),
            pltpu.VMEM((N_CH, 6, 2, rows, CW), F32),
            pltpu.VMEM((6, 2, rows, TAIL), F32),
            pltpu.VMEM((N_CH, 6, rows // 2, CW), F32),
            pltpu.VMEM((6, rows // 2, TAIL), F32),
            pltpu.VMEM((8, 128), F32),
            pltpu.VMEM((8, 128), F32),
            dma((9,)), dma((9,)), dma((9,)), dma((2,)), dma, dma((16,)), dma((16,)), dma((4,)), dma((4,)),
            dma((n, 6)), dma((n, 6)), dma((n, 6)), dma((n, 6)), dma((2, 4)), dma((2, 4)), dma((32,)), dma((32,)), dma((3,)),
        ],
        compiler_params=pltpu.CompilerParams(has_side_effects=True, vmem_limit_bytes=VMEM_LIMIT),
        name="ladder",
    )(tl, vl, v, t2, oo, sw)


def solution(mesh):
    n_row = mesh.shape["row"]
    n_col = mesh.shape["col"]
    amp_spec = P("row", "col")
    wide_spec = P(None, "col")

    def local_sweep(t_blk, d_blk, oovv_blk, vvvv_blk, oooo_full, wd_blk, wx_blk):
        rows_dev, cols_dev = t_blk.shape
        n_occ = math.isqrt(oooo_full.shape[0])
        n_virt = wd_blk.shape[0] // n_occ
        occ_col = n_occ // n_col
        virt_col = n_virt // n_col
        c_dev = vvvv_blk.shape[0]
        n_p = cols_dev // c_dev
        q = lax.axis_index("row") // 2
        core = lax.axis_index("row") % 2
        t_half = t_blk.astype(BF16)
        ts = t_half.reshape(rows_dev, n_p, c_dev).transpose(1, 0, 2)
        vs = oovv_blk.reshape(n_col, occ_col, n_p, c_dev).transpose(2, 0, 1, 3)
        t3 = t_half.reshape(n_occ, virt_col, n_virt)
        l1 = t3.transpose(1, 0, 2).reshape(virt_col, n_occ * n_virt)
        l1 = jnp.pad(l1, ((0, 12), (0, 0)))
        tb = t3.transpose(2, 0, 1)
        odd = lax.axis_index("col") % 2 == 1
        z4 = jnp.zeros((n_virt, n_occ, 4), BF16)
        full = jnp.where(odd, tb[:, :, 4:], tb[:, :, :32]).reshape(n_virt, n_occ * 32)
        edge = jnp.where(odd, jnp.concatenate([z4, tb[:, :, :4]], axis=2), jnp.concatenate([tb[:, :, 32:], z4], axis=2))
        l2 = jnp.concatenate([full, edge.reshape(n_virt, n_occ * 8)], axis=1)
        wd3 = wd_blk.reshape(n_occ, n_virt, occ_col * n_virt)
        wx3 = wx_blk.reshape(n_occ, n_virt, occ_col * n_virt)
        tl, vl, sw = gather_call(ts, l1, l2, vs, wd3, wx3)
        start = q * 2 * n_occ + lax.axis_index("col") * occ_col
        oo = jnp.stack([lax.dynamic_slice_in_dim(oooo_full, start + i * n_occ, occ_col, axis=0) for i in range(2)])
        oo = oo.reshape(2, occ_col, 16, 2, n_occ)
        oo = jnp.where(core == 1, oo[:, :, :, 1], oo[:, :, :, 0]).reshape(2, occ_col, 16 * n_occ)
        ladder_sum, s1, ps = ladder_call(tl, vl, vvvv_blk, t_half, oo, sw)
        s1 = s1[:, :virt_col].reshape(n_col, virt_col, occ_col, n_virt).transpose(0, 2, 1, 3).reshape(n_occ, cols_dev)
        ps = lax.dynamic_slice_in_dim(ps[:, :virt_col], 16 * (lax.axis_index("row") % 8), n_virt, axis=2).reshape(n_occ, cols_dev)
        ph_sym = s1 + ps
        residual = oovv_blk.astype(F32) + ladder_sum + ph_sym
        return residual / d_blk

    return jax.shard_map(local_sweep, mesh=mesh, in_specs=(amp_spec, amp_spec, amp_spec, amp_spec, P(), wide_spec, wide_spec), out_specs=amp_spec, check_vma=False)
```

```python
import math
import jax
import jax.numpy as jnp
from jax import lax
from jax.experimental import pallas as pl
from jax.experimental.pallas import tpu as pltpu
from jax.sharding import PartitionSpec as P

MESH = pl.DeviceIdType.MESH
BF16 = jnp.bfloat16
F32 = jnp.float32
VMEM_LIMIT = 67_043_328
LANE = 128
RING = 4
PLANE = 16
ROWS = 32
FULL = 32
EDGE = 8
N_CH = 10
CW = 512
TAIL = 64


def _place():
    x = lax.axis_index("col")
    r = lax.axis_index("row")
    q = r // 2
    return x, q // RING, q % RING, r % 2, q, r


def _rc(src, dst, ssem, rsem, dev):
    return pltpu.make_async_remote_copy(src_ref=src, dst_ref=dst, send_sem=ssem, recv_sem=rsem, device_id=dev, device_id_type=MESH)


def _enter(x, z, core, r):
    bar = pltpu.get_barrier_semaphore()

    def tell(dev):
        pl.semaphore_signal(bar, inc=1, device_id=dev, device_id_type=MESH)

    for k in range(1, RING):
        tell(((x + k) % RING, r))
    for k in range(1, ROWS):
        tell((x, (r + k) % ROWS))

    @pl.when(x != z)
    def _():
        for k in range(PLANE):
            tell((z, k * 2 + core))

    pl.semaphore_wait(bar, RING - 1 + ROWS - 1 + RING * (RING - 1))


def sweep_kernel(ts, l1, l2, vs, wd, wx, v_hbm, t2, oo, out, s1_in, ps_in,
                 g, tl, vl, lg1, lg2, wdb, wxb, wxs, d_n, e_n, sw, s2_in, v_buf, t_pair, m_t, x_part, x_in, m_all,
                 p_b, p_t, r1, r1t, r2, r2t,
                 g_s, g_r, t_s, t_r, p_s, p_r, o_s, o_r, v_s, v_r, f_s, f_r, loc, wd_s, wx_s, wy_s,
                 vl_s, vx_s, vx_r, tp_s, tp_r, x_s, x_r, m_s, m_r, s1, w1, s2, w2, sw_s, sw_r, ps_s, ps_r):
    x, z, y, core, q, r = _place()
    right, left = (x + 1) % RING, (x + RING - 1) % RING
    mate = (x, q * 2 + 1 - core)
    n_kd, n_v, n_j = wd.shape
    rows, n_c = tl.shape[2:]
    loc_g, loc_t, loc_1, loc_2, loc_v, loc_p, loc_a, loc_b = [loc.at[i] for i in range(loc.shape[0])]
    _enter(x, z, core, r)

    def ring(src, buf, ss, rr, axis):
        h = src.shape[axis] // 2

        def part(i):
            return (pl.ds(i * h, h),) if axis == 0 else (slice(None), pl.ds(i * h, h))

        def hop(i, who, blk, to):
            ref = buf.at[(blk,) + part(i - 2)]
            return _rc(ref, ref, ss.at[i], rr.at[i], (to, who))

        c0 = _rc(src, buf.at[x], ss.at[0], rr.at[0], (right, r))
        c1 = _rc(src, buf.at[x], ss.at[1], rr.at[1], (left, r))
        return c0, c1, lambda: hop(2, r, left, right), lambda: hop(3, r, right, left)

    own = pltpu.make_async_copy(ts, g.at[x], loc_g)
    own1 = pltpu.make_async_copy(l1, lg1.at[x], loc_1)
    own2 = pltpu.make_async_copy(l2, lg2.at[x], loc_2)
    g0, g1, g2, g3 = ring(ts, g, g_s, g_r, 0)
    own.start()
    g0.start()
    g1.start()
    own1.start()
    own2.start()

    def wd_copy(i):
        return pltpu.make_async_copy(wd.at[pl.ds(EDGE * i, EDGE)], wdb.at[i % 2], wd_s.at[i % 2])

    def wx_copy(i):
        c, h = i // 2, n_kd // 2
        src = wx.at[pl.ds(i % 2 * h, h), pl.ds(FULL * c + EDGE * ((c + 1) // 2), FULL)]
        return pltpu.make_async_copy(src, wxb.at[i % 2], wx_s.at[i % 2])

    def wy_copy(i):
        return pltpu.make_async_copy(wx.at[:, pl.ds(FULL + n_v // 2 * i, EDGE)], wxs.at[i], wy_s.at[i])

    for i in range(2):
        wd_copy(i).start()
        wx_copy(i).start()
        wy_copy(i).start()

    def v_copy(x2, yd):
        return _rc(vs.at[pl.ds(2 * yd, 2), x2], vl.at[:, core, q], v_s.at[x2, yd], v_r.at[q], (x2, (x * RING + yd) * 2 + core))

    def v_arrival(k):
        return _rc(vs.at[pl.ds(2 * y, 2), x], vl.at[:, core, (q + k) % PLANE], v_s.at[x, y], v_r.at[(q + k) % PLANE], (x, r))

    v_own = pltpu.make_async_copy(vs.at[pl.ds(2 * y, 2), x], vl.at[:, core, q], loc_v)

    def v_each(act, act_own):
        for i in range(RING):
            for k in range(RING):
                c = v_copy((x + i) % RING, (y + k) % RING)
                if i + k == 0:
                    if act_own is not None:
                        pl.when(x == z)(act_own)
                    pl.when(x != z)(lambda: act(c))
                else:
                    act(c)

    def t_copy(xs, yd):
        return _rc(g.at[xs, pl.ds(2 * yd, 2)], tl.at[:, q], t_s.at[xs, yd], t_r.at[q], (x, (xs * RING + yd) * 2 + core))

    def t_arrival(k):
        return _rc(g.at[x, pl.ds(2 * y, 2)], tl.at[:, (q + k) % PLANE], t_s.at[x, y], t_r.at[(q + k) % PLANE], (x, r))

    def t_block(rel):
        xs = (x + rel) % RING
        for k in range(RING):
            yd = (y + k) % RING
            if k == 0:
                pl.when(xs == z)(lambda: pltpu.make_async_copy(g.at[xs, pl.ds(2 * yd, 2)], tl.at[:, q], loc_t).start())
                pl.when(xs != z)(lambda: t_copy(xs, yd).start())
            else:
                t_copy(xs, yd).start()

    own.wait()
    t_block(0)
    v_each(lambda c: c.start(), v_own.start)
    g0.wait_recv()
    g2 = g2()
    g2.start()
    t_block(RING - 1)
    g1.wait_recv()
    g3 = g3()
    g3.start()
    t_block(1)
    a0, a1, a2, a3 = ring(l1, lg1, p_s, p_r, 1)
    b0, b1, b2, b3 = ring(l2, lg2, o_s, o_r, 1)
    for c in (a0, a1, b0, b1):
        c.start()
    g2.wait_recv()
    g3.wait_recv()
    t_block(2)

    n_v9 = vl_s.shape[0]
    wide = 640
    v_in = []
    for i in range(n_v9):
        c0 = i * wide
        w = min(wide, v_hbm.shape[1] - c0)
        src, dst = v_hbm.at[:, pl.ds(c0, w)], v_buf.at[core, :, pl.ds(c0, w)]
        v_in += [pltpu.make_async_copy(src, dst, vl_s.at[i]), _rc(src, dst, vx_s.at[i], vx_r.at[i], mate)]
    v_in += [pltpu.make_async_copy(t2, t_pair.at[core], loc_p), _rc(t2, t_pair.at[core], tp_s, tp_r, mate)]
    for c in v_in:
        c.start()

    pl.when(x == z)(v_own.wait)
    pl.when(x != z)(lambda: v_arrival(0).wait_recv())
    for k in range(1, PLANE):
        v_arrival(k).wait_recv()
    fwd = _rc(vl.at[:, core], vl.at[:, core], f_s, f_r, mate)
    fwd.start()
    a0.wait_recv()
    a2 = a2()
    a2.start()
    a1.wait_recv()
    a3 = a3()
    a3.start()
    pltpu.make_async_copy(g.at[x, pl.ds(2 * y, 2)], tl.at[:, q], loc_t).wait()
    for k in range(1, PLANE):
        t_arrival(k).wait_recv()
    fwd.wait()

    k8 = vl.shape[3]
    n_i = PLANE * rows
    n_k = 2 * PLANE * k8
    dn = (((1,), (1,)), ((), ()))
    xp = [lax.dot_general(vl[i].reshape(n_k, n_c), tl[i].reshape(n_i, n_c), dn, preferred_element_type=F32) for i in range(2)]
    x_part[...] = (xp[0] + xp[1]).reshape(2, PLANE, k8, n_i)

    def x_copy(k):
        qd = (q + k) % PLANE
        return _rc(x_part.at[:, qd], x_in.at[q], x_s.at[k], x_r.at[k], (x, qd * 2 + core))

    for k in range(1, PLANE):
        x_copy(k).start()
    x_in[q] = x_part[:, q]
    b0.wait_recv()
    b2 = b2()
    b2.start()
    b1.wait_recv()
    b3 = b3()
    b3.start()

    n1 = l1.shape[0]
    quarter = n_v // RING
    own1.wait()
    own2.wait()
    a2.wait_recv()
    a3.wait_recv()
    acc = None
    for i in range(RING):
        wd_copy(i).wait()
        lhs = lg1[:, :, i * EDGE * n_v:(i + 1) * EDGE * n_v].reshape(RING * n1, EDGE * n_v)
        d = jnp.dot(lhs, wdb[i % 2].reshape(EDGE * n_v, n_j), preferred_element_type=F32)
        acc = d if acc is None else acc + d
        if i < 2:
            wd_copy(i + 2).start()
    for i in range(RING):
        d_n[quarter * i:quarter * (i + 1), :] = acc[n1 * i:n1 * i + quarter]
    b2.wait_recv()
    b3.wait_recv()
    acc = None
    kb = FULL * n_kd
    kh = kb // 2
    for i in range(2 * RING):
        wx_copy(i).wait()
        d = jnp.dot(lg2[i // 2, :, i % 2 * kh:(i % 2 + 1) * kh], wxb[i % 2].reshape(kh, n_j), preferred_element_type=F32)
        acc = d if acc is None else acc + d
        if i + 2 < 2 * RING:
            wx_copy(i + 2).start()
    for i in range(2):
        wy_copy(i).wait()
        lhs = lg2[2 * i, :, kb:] + lg2[2 * i + 1, :, kb:]
        acc = acc + jnp.dot(lhs, wxs[i].reshape(EDGE * n_kd, n_j), preferred_element_type=F32)
    e_n[...] = acc

    for k in range(1, PLANE):
        x_copy(k).wait_recv()
    xs = x_in[0]
    for k in range(1, PLANE):
        xs = xs + x_in[k]
    m_all[x] = (oo[...].astype(F32) + 0.5 * xs).astype(BF16)

    def m_copy(k):
        return _rc(m_all.at[x], m_all.at[x], m_s.at[k], m_r.at[k], ((x + k) % RING, r))

    for k in range(1, RING):
        m_copy(k).start()

    for j in range(n_j // n_v):
        cut = slice(j * n_v, (j + 1) * n_v)
        sj = d_n[:, cut] - e_n[:, cut].T
        d_n[:, cut] = sj
        e_n[:, cut] = sj.T
    for i in range(RING):
        sw[0, i, :quarter, :] = d_n[quarter * i:quarter * (i + 1), :]
        sw[1, i, :quarter, :] = e_n[quarter * i:quarter * (i + 1), :]

    def s_copy(i, k):
        xd = (x + k) % RING
        return _rc(sw.at[i, xd], (s1_in, s2_in)[i].at[x], sw_s.at[i, k], sw_r.at[i, k], (xd, r))

    s_own = [pltpu.make_async_copy(sw.at[i, x], (s1_in, s2_in)[i].at[x], (loc_a, loc_b)[i]) for i in range(2)]
    for i in (1, 0):
        for k in range(1, RING):
            s_copy(i, k).start()
        s_own[i].start()

    def ps_src(rd):
        return s2_in.at[rd // EDGE, :, pl.ds(pl.multiple_of(rd % EDGE * 9 // EDGE * LANE, LANE), 2 * LANE)]

    def ps_copy(k):
        rd = (r + k) % ROWS
        return _rc(ps_src(rd), ps_in.at[r], ps_s.at[k], ps_r.at[k], (x, rd))

    ps_own = pltpu.make_async_copy(ps_src(r), ps_in.at[r], loc_g)

    def ps_send():
        s_own[1].wait()
        for k in range(1, RING):
            s_copy(1, k).wait_recv()
        ps_own.start()
        for k in range(1, ROWS):
            ps_copy(k).start()

    for c in v_in:
        c.wait()
    for k in range(1, RING):
        m_copy(k).wait_recv()
    mf = m_all[...].astype(F32)
    m_t[...] = jnp.concatenate([mf[xx, cc] for cc in range(2) for xx in range(RING)], axis=0).T.astype(BF16)

    def to(first, a, d):
        b = a if first else 1 - a
        return (x, (((z + d * (1 - b)) % RING) * RING + (y + d * b) % RING) * 2 + core)

    def coords(a):
        return y * a + z * (1 - a), z * a + y * (1 - a)

    def stage(first, t, a, pb, rb):
        u, v = coords(a)
        c, pre, n = (u, (), 2) if first else (v, (u,), rows // 2)
        lo, hi = pl.ds(0, n), pl.ds(n, n)
        far, up, dn_ = (c + 2) % RING, (c + 1) % RING, (c + RING - 1) % RING
        ss, ww = (s1, w1) if first else (s2, w2)
        srcs = (far, lo), (far, hi), (up, hi), (dn_, lo), (up, lo), (dn_, hi)

        def msg(i):
            d = 1 if i % 2 == 0 else RING - 1
            return _rc(pb.at[pre + srcs[i]], rb.at[i], ss.at[t, i], ww.at[t, i], to(first, a, d))
        return msg

    near = range(2, 6)

    def l1_step(t, a, pb, rb, c0, w):
        tp = t_pair[:, :, pl.ds(c0, w)].reshape(2 * rows, w)
        acc = jnp.dot(m_t[...], tp, preferred_element_type=F32)
        for i in range(2):
            acc = acc + jnp.dot(tl[i].reshape(n_i, n_c), v_buf[i, :, pl.ds(c0, w)], preferred_element_type=F32)
        for zb in range(RING):
            for yb in range(RING):
                b = (zb * RING + yb) * rows
                pb[yb * a + zb * (1 - a), zb * a + yb * (1 - a)] = acc[b:b + rows]
        msg = stage(True, t, a, pb, rb)
        for i in range(4):
            msg(i).start()

    def add_step(first, t, a, pb, rb):
        u, v = coords(a)
        c, pre, n = (u, (), 2) if first else (v, (u,), rows // 2)
        msg = stage(first, t, a, pb, rb)
        msg(0).wait_recv()
        up = pre + ((c + 1) % RING, pl.ds(0, n))
        pb[up] = pb[up] + rb[0]
        msg(4).start()
        msg(1).wait_recv()
        dn_ = pre + ((c + RING - 1) % RING, pl.ds(n, n))
        pb[dn_] = pb[dn_] + rb[1]
        msg(5).start()

    def l3_step(t, a, pb, rb, rb2):
        u, _ = coords(a)
        msg = stage(True, t, a, pb, rb)
        for i in near:
            msg(i).wait_recv()
        pb[u, :2] = pb[u, :2] + rb[4] + rb[3]
        pb[u, 2:] = pb[u, 2:] + rb[2] + rb[5]
        nxt = stage(False, t, a, pb, rb2)
        for i in range(4):
            nxt(i).start()

    def l5_step(t, a, pb, rb, rb2, c0, w):
        u, v = coords(a)
        h = rows // 2
        msg, old = stage(False, t, a, pb, rb2), stage(True, t, a, pb, rb)
        for i in near:
            msg(i).wait_recv()
        out[:h, pl.ds(c0, w)] = pb[u, v, :h] + rb2[4] + rb2[3]
        out[h:, pl.ds(c0, w)] = pb[u, v, h:] + rb2[2] + rb2[5]
        for i in range(6):
            msg(i).wait_send()
            old(i).wait_send()

    def at(t):
        return (t, 1 - t % 2, p_b.at[t], r1.at[t], r2.at[t])

    def col0(t):
        return pl.multiple_of((t // 2) * CW + (t % 2) * (N_CH // 2) * CW, LANE)

    def loop(lo, fn):
        lax.fori_loop(lo, N_CH, lambda t, c: (fn(t), c)[1], 0)

    tail = (N_CH, 1, p_t, r1t, r2t)
    ct = N_CH * CW

    def run1(t):
        n, a, pb, rb, _ = at(t)
        l1_step(n, a, pb, rb, col0(t), CW)

    def run3(t):
        l3_step(*at(t))
        n, a, pb, _, rb2 = at(t - 1)
        add_step(False, n, a, pb, rb2)

    l1_step(*tail[:4], ct, TAIL)
    loop(0, run1)
    ps_send()
    add_step(True, *tail[:4])
    loop(0, lambda t: add_step(True, *at(t)[:4]))
    l3_step(*tail)
    add_step(False, *tail[:3], r2t)
    l3_step(*at(0))
    loop(1, run3)
    n, a, pb, _, rb2 = at(N_CH - 1)
    add_step(False, n, a, pb, rb2)
    l5_step(*tail, ct, TAIL)
    loop(0, lambda t: l5_step(*at(t), col0(t), CW))

    for c in (g0, g1, g2, g3, a0, a1, a2, a3, b0, b1, b2, b3):
        c.wait_send()
    for rel in range(RING):
        xs = (x + rel) % RING
        for k in range(RING):
            c = t_copy(xs, (y + k) % RING)
            if k == 0:
                pl.when(xs != z)(c.wait_send)
            else:
                c.wait_send()
    v_each(lambda c: c.wait_send(), None)
    for k in range(1, PLANE):
        x_copy(k).wait_send()
    for k in range(1, RING):
        m_copy(k).wait_send()
        s_copy(0, k).wait()
        s_copy(1, k).wait_send()
    s_own[0].wait()
    ps_own.wait()
    for k in range(1, ROWS):
        ps_copy(k).wait()


def sweep_call(ts, l1, l2, vs, wd, wx, v, t2, oo):
    n_p, rows, n_c = ts.shape
    n_k, n_v, n_j = wd.shape
    cols = t2.shape[1]
    k8 = rows // RING
    n_i = PLANE * rows
    blk = (n_v // RING + RING, n_j)
    n = N_CH + 1
    dma = pltpu.SemaphoreType.DMA
    vm = pl.BlockSpec(memory_space=pltpu.VMEM)
    hbm = pl.BlockSpec(memory_space=pl.ANY)

    def b16(*shape):
        return pltpu.VMEM(shape, BF16)

    def f32(*shape):
        return pltpu.VMEM(shape, F32)

    def sems(*shape):
        return dma(shape)

    one, two, four, six = (), (2,), (RING,), (n, 6)
    all16, sq = (PLANE,), (RING, RING)
    v9 = (-(-cols // 640),)
    counts = [four, four, sq, all16, four, four, four, four, sq, all16, one, one, (8,), two, two, two,
              v9, v9, v9, one, one, all16, all16, four, four, six, six, six, six, (2, RING), (2, RING), (ROWS,), (ROWS,)]
    return pl.pallas_call(
        sweep_kernel,
        out_shape=[
            jax.ShapeDtypeStruct((rows, cols), F32),
            jax.ShapeDtypeStruct((RING,) + blk, F32),
            jax.ShapeDtypeStruct((ROWS, blk[0], 2 * LANE), F32),
        ],
        in_specs=[vm, vm, vm, vm, hbm, hbm, hbm, vm, vm],
        out_specs=[vm, vm, vm],
        scratch_shapes=[
            b16(RING, n_p, rows, n_c), b16(2, PLANE, rows, n_c), b16(2, 2, PLANE, k8, n_c),
            b16(RING, *l1.shape), b16(RING, *l2.shape),
            b16(2, EDGE, n_v, n_j), b16(2, n_k // 2, FULL, n_j), b16(2, n_k, EDGE, n_j),
            f32(n_v, n_j), f32(n_v, n_j), f32(2, RING, *blk), f32(RING, *blk),
            b16(2, n_c, cols), b16(2, rows, cols), b16(n_i, 2 * rows),
            f32(2, PLANE, k8, n_i), f32(PLANE, 2, k8, n_i), b16(RING, 2, k8, n_i),
            f32(N_CH, RING, RING, rows, CW), f32(RING, RING, rows, TAIL),
            f32(N_CH, 6, 2, rows, CW), f32(6, 2, rows, TAIL),
            f32(N_CH, 6, rows // 2, CW), f32(6, rows // 2, TAIL),
        ] + [sems(*c) if c else dma for c in counts],
        compiler_params=pltpu.CompilerParams(has_side_effects=True, collective_id=0, vmem_limit_bytes=VMEM_LIMIT),
        name="sweep",
    )(ts, l1, l2, vs, wd, wx, v, t2, oo)


def solution(mesh):
    n_col = mesh.shape["col"]
    amp_spec = P("row", "col")
    wide_spec = P(None, "col")

    def local_sweep(t_blk, d_blk, oovv_blk, vvvv_blk, oooo_full, wd_blk, wx_blk):
        rows_dev, cols_dev = t_blk.shape
        n_occ = math.isqrt(oooo_full.shape[0])
        n_virt = wd_blk.shape[0] // n_occ
        occ_col = n_occ // n_col
        virt_col = n_virt // n_col
        c_dev = vvvv_blk.shape[0]
        n_p = cols_dev // c_dev
        x = lax.axis_index("col")
        r = lax.axis_index("row")
        t_half = t_blk.astype(BF16)
        ts = t_half.reshape(rows_dev, n_p, c_dev).transpose(1, 0, 2)
        vs = oovv_blk.reshape(n_col, occ_col, n_p, c_dev).transpose(2, 0, 1, 3)
        t3 = t_half.reshape(n_occ, virt_col, n_virt)
        l1 = t3.transpose(1, 0, 2).reshape(virt_col, n_occ * n_virt)
        l1 = jnp.pad(l1, ((0, 12), (0, 0)))
        tb = t3.transpose(2, 0, 1)
        odd = x % 2 == 1
        rest = virt_col - FULL
        gap = jnp.zeros((n_virt, n_occ, EDGE - rest), BF16)
        full = jnp.where(odd, tb[:, :, rest:], tb[:, :, :FULL]).reshape(n_virt, n_occ * FULL)
        edge = jnp.where(odd, jnp.concatenate([gap, tb[:, :, :rest]], axis=2), jnp.concatenate([tb[:, :, FULL:], gap], axis=2))
        l2 = jnp.concatenate([full, edge.reshape(n_virt, n_occ * EDGE)], axis=1)
        wd3 = wd_blk.reshape(n_occ, n_virt, occ_col * n_virt)
        wx3 = wx_blk.reshape(n_occ, n_virt, occ_col * n_virt)
        start = r // 2 * 2 * n_occ + x * occ_col
        oo = jnp.stack([lax.dynamic_slice_in_dim(oooo_full, start + i * n_occ, occ_col, axis=0) for i in range(2)])
        oo = oo.reshape(2, occ_col, PLANE, 2, n_occ)
        oo = jnp.where(r % 2 == 1, oo[:, :, :, 1], oo[:, :, :, 0]).reshape(2, occ_col, PLANE * n_occ)
        ladder_sum, s1, ps = sweep_call(ts, l1, l2, vs, wd3, wx3, vvvv_blk, t_half, oo)
        s1 = s1[:, :virt_col].reshape(n_col, virt_col, occ_col, n_virt).transpose(0, 2, 1, 3).reshape(n_occ, cols_dev)
        ps = lax.dynamic_slice_in_dim(ps[:, :virt_col], PLANE * (r % EDGE), n_virt, axis=2).reshape(n_occ, cols_dev)
        ph_sym = s1 + ps
        residual = oovv_blk.astype(F32) + ladder_sum + ph_sym
        return residual / d_blk

    return jax.shard_map(local_sweep, mesh=mesh, in_specs=(amp_spec, amp_spec, amp_spec, amp_spec, P(), wide_spec, wide_spec), out_specs=amp_spec, check_vma=False)
```

```python
import math
import jax
import jax.numpy as jnp
from jax import lax
from jax.experimental import pallas as pl
from jax.experimental.pallas import tpu as pltpu
from jax.sharding import PartitionSpec as P

MESH = pl.DeviceIdType.MESH
BF16 = jnp.bfloat16
F32 = jnp.float32
VMEM_LIMIT = 67_043_328
LANE = 128
RING = 4
PLANE = 16
ROWS = 32
FULL = 32
EDGE = 8
N_CH = 10
EARLY = 3
CW = 512
TAIL = 64


def _place():
    x = lax.axis_index("col")
    r = lax.axis_index("row")
    q = r // 2
    return x, q // RING, q % RING, r % 2, q, r


def _rc(src, dst, ssem, rsem, dev):
    return pltpu.make_async_remote_copy(src_ref=src, dst_ref=dst, send_sem=ssem, recv_sem=rsem, device_id=dev, device_id_type=MESH)


def _enter(x, z, core, r):
    bar = pltpu.get_barrier_semaphore()

    def tell(dev):
        pl.semaphore_signal(bar, inc=1, device_id=dev, device_id_type=MESH)

    for k in range(1, RING):
        tell(((x + k) % RING, r))
    for k in range(1, ROWS):
        tell((x, (r + k) % ROWS))

    @pl.when(x != z)
    def _():
        for k in range(PLANE):
            tell((z, k * 2 + core))

    pl.semaphore_wait(bar, RING - 1 + ROWS - 1 + RING * (RING - 1))


def sweep_kernel(ts, l1, l2, vs, wd, wx, v_hbm, t2, oo_hbm, out_hbm,
                 g, tl, vl, lg1, lg2, wdb, wxb, wxs, d_n, e_n, s_f, s_b, sw, s1_in, s2_in, ps_in, out, oo2, oo, v_buf, t_pair, m_t, x_part, x_in, m_all,
                 p_b, p_t, r1, r1t, r2, r2t,
                 g_s, g_r, t_s, t_r, p_s, p_r, o_s, o_r, v_s, v_r, f_s, f_r, loc, wd_s, wx_s, wy_s,
                 vl_s, vx_s, vx_r, tp_s, tp_r, x_s, x_r, m_s, m_r, s1, w1, s2, w2, sw_s, sw_r, ps_s, ps_r, out_s, oo_s):
    x, z, y, core, q, r = _place()
    right, left = (x + 1) % RING, (x + RING - 1) % RING
    mate = (x, q * 2 + 1 - core)
    n_kd, n_v, n_j = wd.shape
    rows, n_c = tl.shape[2:]
    loc_g, loc_t, loc_1, loc_2, loc_v, loc_p, loc_a, loc_b = [loc.at[i] for i in range(loc.shape[0])]
    _enter(x, z, core, r)

    def ring(src, buf, ss, rr, axis):
        h = src.shape[axis] // 2

        def part(i):
            return (pl.ds(i * h, h),) if axis == 0 else (slice(None), pl.ds(i * h, h))

        def hop(i, who, blk, to):
            ref = buf.at[(blk,) + part(i - 2)]
            return _rc(ref, ref, ss.at[i], rr.at[i], (to, who))

        c0 = _rc(src, buf.at[x], ss.at[0], rr.at[0], (right, r))
        c1 = _rc(src, buf.at[x], ss.at[1], rr.at[1], (left, r))
        return c0, c1, lambda: hop(2, r, left, right), lambda: hop(3, r, right, left)

    own = pltpu.make_async_copy(ts, g.at[x], loc_g)
    own1 = pltpu.make_async_copy(l1, lg1.at[x], loc_1)
    own2 = pltpu.make_async_copy(l2, lg2.at[x], loc_2)
    g0, g1, g2, g3 = ring(ts, g, g_s, g_r, 0)
    own.start()
    g0.start()
    g1.start()
    own1.start()
    own2.start()

    def wd_copy(i):
        return pltpu.make_async_copy(wd.at[pl.ds(RING * i, RING)], wdb.at[i % 2], wd_s.at[i % 2])

    def wx_copy(i):
        c, h = i // 2, n_kd // 2
        src = wx.at[pl.ds(i % 2 * h, h), pl.ds(FULL * c + EDGE * ((c + 1) // 2), FULL)]
        return pltpu.make_async_copy(src, wxb.at[i % 2], wx_s.at[i % 2])

    def wy_copy(i):
        return pltpu.make_async_copy(wx.at[:, pl.ds(FULL + n_v // 2 * i, EDGE)], wxs.at[i], wy_s.at[i])

    def oo_copy(i):
        k0 = pl.multiple_of((2 * q + i) * rows + x * EDGE, EDGE)
        return pltpu.make_async_copy(oo_hbm.at[pl.ds(k0, EDGE)], oo2.at[i], oo_s.at[i])

    for i in range(2):
        oo_copy(i).start()
        wd_copy(i).start()
        wx_copy(i).start()
        wy_copy(i).start()

    def v_copy(x2, yd):
        return _rc(vs.at[pl.ds(2 * yd, 2), x2], vl.at[:, core, q], v_s.at[x2, yd], v_r.at[q], (x2, (x * RING + yd) * 2 + core))

    def v_arrival(k):
        return _rc(vs.at[pl.ds(2 * y, 2), x], vl.at[:, core, (q + k) % PLANE], v_s.at[x, y], v_r.at[(q + k) % PLANE], (x, r))

    v_own = pltpu.make_async_copy(vs.at[pl.ds(2 * y, 2), x], vl.at[:, core, q], loc_v)

    def v_each(act, act_own):
        for i in range(RING):
            for k in range(RING):
                c = v_copy((x + i) % RING, (y + k) % RING)
                if i + k == 0:
                    if act_own is not None:
                        pl.when(x == z)(act_own)
                    pl.when(x != z)(lambda: act(c))
                else:
                    act(c)

    def t_copy(xs, yd):
        return _rc(g.at[xs, pl.ds(2 * yd, 2)], tl.at[:, q], t_s.at[xs, yd], t_r.at[q], (x, (xs * RING + yd) * 2 + core))

    def t_arrival(k):
        return _rc(g.at[x, pl.ds(2 * y, 2)], tl.at[:, (q + k) % PLANE], t_s.at[x, y], t_r.at[(q + k) % PLANE], (x, r))

    def t_block(rel):
        xs = (x + rel) % RING
        for k in range(RING):
            yd = (y + k) % RING
            if k == 0:
                pl.when(xs == z)(lambda: pltpu.make_async_copy(g.at[xs, pl.ds(2 * yd, 2)], tl.at[:, q], loc_t).start())
                pl.when(xs != z)(lambda: t_copy(xs, yd).start())
            else:
                t_copy(xs, yd).start()

    own.wait()
    t_block(0)
    g0.wait_recv()
    g2 = g2()
    g2.start()
    t_block(RING - 1)
    g1.wait_recv()
    g3 = g3()
    g3.start()
    v_each(lambda c: c.start(), v_own.start)
    t_block(1)
    a0, a1, a2, a3 = ring(l1, lg1, p_s, p_r, 1)
    b0, b1, b2, b3 = ring(l2, lg2, o_s, o_r, 1)
    for c in (a0, a1, b0, b1):
        c.start()
    g2.wait_recv()
    g3.wait_recv()
    t_block(2)

    n_v9 = vl_s.shape[0]
    wide = 640
    v_in = []
    for i in range(n_v9):
        c0 = i * wide
        w = min(wide, v_hbm.shape[1] - c0)
        src, dst = v_hbm.at[:, pl.ds(c0, w)], v_buf.at[core, :, pl.ds(c0, w)]
        v_in += [pltpu.make_async_copy(src, dst, vl_s.at[i]), _rc(src, dst, vx_s.at[i], vx_r.at[i], mate)]
    v_in += [pltpu.make_async_copy(t2, t_pair.at[core], loc_p), _rc(t2, t_pair.at[core], tp_s, tp_r, mate)]
    for c in v_in:
        c.start()

    for i in range(2):
        oo_copy(i).wait()
    ow = oo2[...].astype(F32)
    for k in range(PLANE):
        c0 = 2 * k * rows
        oo[:, :, k * rows:(k + 1) * rows] = jnp.where(core == 1, ow[:, :, c0 + rows:c0 + 2 * rows], ow[:, :, c0:c0 + rows])

    pl.when(x == z)(v_own.wait)
    pl.when(x != z)(lambda: v_arrival(0).wait_recv())
    for k in range(1, PLANE):
        v_arrival(k).wait_recv()
    fwd = _rc(vl.at[:, core], vl.at[:, core], f_s, f_r, mate)
    fwd.start()

    pltpu.make_async_copy(g.at[x, pl.ds(2 * y, 2)], tl.at[:, q], loc_t).wait()
    for k in range(1, PLANE):
        t_arrival(k).wait_recv()
    fwd.wait()

    k8 = vl.shape[3]
    n_i = PLANE * rows
    n_k = 2 * PLANE * k8
    dn = (((1,), (1,)), ((), ()))
    xp = [lax.dot_general(vl[i].reshape(n_k, n_c), tl[i].reshape(n_i, n_c), dn, preferred_element_type=F32) for i in range(2)]
    x_part[...] = (xp[0] + xp[1]).reshape(2, PLANE, k8, n_i)

    def x_copy(k):
        qd = (q + k) % PLANE
        return _rc(x_part.at[:, qd], x_in.at[q], x_s.at[k], x_r.at[k], (x, qd * 2 + core))

    for k in range(1, PLANE):
        x_copy(k).start()
    x_in[q] = x_part[:, q]
    a0.wait_recv()
    a2 = a2()
    a2.start()
    a1.wait_recv()
    a3 = a3()
    a3.start()
    b0.wait_recv()
    b2 = b2()
    b2.start()
    b1.wait_recv()
    b3 = b3()
    b3.start()

    for k in range(1, PLANE):
        x_copy(k).wait_recv()
    xs = x_in[0]
    for k in range(1, PLANE):
        xs = xs + x_in[k]
    m_all[x] = (oo[...] + 0.5 * xs).astype(BF16)

    def m_copy(k):
        return _rc(m_all.at[x], m_all.at[x], m_s.at[k], m_r.at[k], ((x + k) % RING, r))

    for k in range(1, RING):
        m_copy(k).start()

    def s_copy(i, k):
        xd = (x + k) % RING
        return _rc(sw.at[i, xd], (s1_in, s2_in)[i].at[x], sw_s.at[i, k], sw_r.at[i, k], (xd, r))

    s_own = [pltpu.make_async_copy(sw.at[i, x], (s1_in, s2_in)[i].at[x], (loc_a, loc_b)[i]) for i in range(2)]
    def ps_src(rd):
        return s2_in.at[rd // EDGE, pl.ds(rd % EDGE, 1)]

    def ps_copy(k):
        rd = (r + k) % ROWS
        return _rc(ps_src(rd), ps_in.at[pl.ds(r, 1)], ps_s.at[k], ps_r.at[k], (x, rd))

    ps_own = pltpu.make_async_copy(ps_src(r), ps_in.at[pl.ds(r, 1)], loc_g)

    def ps_ready():
        s_own[1].wait()
        for k in range(1, RING):
            s_copy(1, k).wait_recv()
        ps_own.start()

    def ps_send(lo, hi):
        for k in range(lo, hi):
            ps_copy(k).start()

    def s_work():
        n1 = l1.shape[0]
        quarter = n_v // RING
        own1.wait()
        own2.wait()
        a2.wait_recv()
        a3.wait_recv()
        acc = None
        kd = RING * n_v
        for i in range(2 * RING):
            wd_copy(i).wait()
            lhs = lg1[:, :, i * kd:(i + 1) * kd].reshape(RING * n1, kd)
            d = jnp.dot(lhs, wdb[i % 2].reshape(kd, n_j), preferred_element_type=F32)
            acc = d if acc is None else acc + d
            if i + 2 < 2 * RING:
                wd_copy(i + 2).start()
        for i in range(RING):
            d_n[quarter * i:quarter * (i + 1), :] = acc[n1 * i:n1 * i + quarter]
        b2.wait_recv()
        b3.wait_recv()
        acc = None
        kb = FULL * n_kd
        kh = kb // 2
        for i in range(2 * RING):
            wx_copy(i).wait()
            d = jnp.dot(lg2[i // 2, :, i % 2 * kh:(i % 2 + 1) * kh], wxb[i % 2].reshape(kh, n_j), preferred_element_type=F32)
            acc = d if acc is None else acc + d
            if i + 2 < 2 * RING:
                wx_copy(i + 2).start()
        for i in range(2):
            wy_copy(i).wait()
            lhs = lg2[2 * i, :, kb:] + lg2[2 * i + 1, :, kb:]
            acc = acc + jnp.dot(lhs, wxs[i].reshape(EDGE * n_kd, n_j), preferred_element_type=F32)
        e_n[...] = acc

        for j in range(n_j // n_v):
            cut = slice(j * n_v, (j + 1) * n_v)
            sj = d_n[:, cut] - e_n[:, cut].T
            s_f[j] = sj
            s_b[j] = sj.T
        for i in range(2):
            for a in range(n_v):
                c0 = a % quarter * n_v
                sw[i, a // quarter, :, c0:c0 + n_v] = (s_f, s_b)[i][:, a, :]
        for i in (1, 0):
            for k in range(1, RING):
                s_copy(i, k).start()
            s_own[i].start()


    for c in v_in:
        c.wait()
    for k in range(1, RING):
        m_copy(k).wait_recv()
    mf = m_all[...].astype(F32)
    m_t[...] = jnp.concatenate([mf[xx, cc] for cc in range(2) for xx in range(RING)], axis=0).T.astype(BF16)

    def to(first, a, d):
        b = a if first else 1 - a
        return (x, (((z + d * (1 - b)) % RING) * RING + (y + d * b) % RING) * 2 + core)

    def coords(a):
        return y * a + z * (1 - a), z * a + y * (1 - a)

    def stage(first, t, a, pb, rb):
        u, v = coords(a)
        c, pre, n = (u, (), 2) if first else (v, (u,), rows // 2)
        lo, hi = pl.ds(0, n), pl.ds(n, n)
        far, up, dn_ = (c + 2) % RING, (c + 1) % RING, (c + RING - 1) % RING
        ss, ww = (s1, w1) if first else (s2, w2)
        srcs = (far, lo), (far, hi), (up, hi), (dn_, lo), (up, lo), (dn_, hi)

        def msg(i):
            d = 1 if i % 2 == 0 else RING - 1
            return _rc(pb.at[pre + srcs[i]], rb.at[i], ss.at[t, i], ww.at[t, i], to(first, a, d))
        return msg

    near = range(2, 6)

    def l1_step(t, a, pb, rb, c0, w):
        tp = t_pair[:, :, pl.ds(c0, w)].reshape(2 * rows, w)
        acc = jnp.dot(m_t[...], tp, preferred_element_type=F32)
        for i in range(2):
            acc = acc + jnp.dot(tl[i].reshape(n_i, n_c), v_buf[i, :, pl.ds(c0, w)], preferred_element_type=F32)
        for zb in range(RING):
            for yb in range(RING):
                b = (zb * RING + yb) * rows
                pb[yb * a + zb * (1 - a), zb * a + yb * (1 - a)] = acc[b:b + rows]
        msg = stage(True, t, a, pb, rb)
        for i in range(4):
            msg(i).start()

    def add_step(first, t, a, pb, rb):
        u, v = coords(a)
        c, pre, n = (u, (), 2) if first else (v, (u,), rows // 2)
        msg = stage(first, t, a, pb, rb)
        msg(0).wait_recv()
        up = pre + ((c + 1) % RING, pl.ds(0, n))
        pb[up] = pb[up] + rb[0]
        msg(4).start()
        msg(1).wait_recv()
        dn_ = pre + ((c + RING - 1) % RING, pl.ds(n, n))
        pb[dn_] = pb[dn_] + rb[1]
        msg(5).start()

    def l3_step(t, a, pb, rb, rb2):
        u, _ = coords(a)
        msg = stage(True, t, a, pb, rb)
        for i in near:
            msg(i).wait_recv()
        pb[u, :2] = pb[u, :2] + rb[4] + rb[3]
        pb[u, 2:] = pb[u, 2:] + rb[2] + rb[5]
        nxt = stage(False, t, a, pb, rb2)
        for i in range(4):
            nxt(i).start()

    def o_copy(t, c0, w):
        return pltpu.make_async_copy(out.at[:, pl.ds(c0, w)], out_hbm.at[:, pl.ds(c0, w)], out_s.at[t])

    def l5_step(t, a, pb, rb, rb2, c0, w):
        u, v = coords(a)
        h = rows // 2
        msg, old = stage(False, t, a, pb, rb2), stage(True, t, a, pb, rb)
        for i in near:
            msg(i).wait_recv()
        sym = s1_in[:, :, pl.ds(c0, w)].reshape(rows, w) + ps_in[:, pl.ds(c0, w)]
        out[:h, pl.ds(c0, w)] = pb[u, v, :h] + rb2[4] + rb2[3] + sym[:h]
        out[h:, pl.ds(c0, w)] = pb[u, v, h:] + rb2[2] + rb2[5] + sym[h:]
        o_copy(t, c0, w).start()
        for i in range(6):
            msg(i).wait_send()
            old(i).wait_send()

    def at(t):
        return (t, 1 - t % 2, p_b.at[t], r1.at[t], r2.at[t])

    def col0(t):
        return pl.multiple_of((t // 2) * CW + (t % 2) * (N_CH // 2) * CW, LANE)

    def loop(lo, fn, hi=N_CH):
        lax.fori_loop(lo, hi, lambda t, c: (fn(t), c)[1], 0)

    tail = (N_CH, 1, p_t, r1t, r2t)
    ct = N_CH * CW

    def each(p, fn):
        for i in range(2):
            fn(2 * p + i)

    def run1(t):
        n, a, pb, rb, _ = at(t)
        l1_step(n, a, pb, rb, col0(t), CW)

    def run2(t):
        add_step(True, *at(t)[:4])

    def run3(t):
        l3_step(*at(t))

    def run4(t):
        n, a, pb, _, rb2 = at(t)
        add_step(False, n, a, pb, rb2)

    pairs = N_CH // 2
    loop(0, run1, 2 * EARLY)
    l1_step(*tail[:4], ct, TAIL)
    s_work()
    add_step(True, *tail[:4])

    def pair_step(p):
        each(p, run2)
        pl.when(p + EARLY < pairs)(lambda: each(p + EARLY, run1))
        pl.when(p >= 1)(lambda: each(p - 1, run3))
        pl.when(p >= 2)(lambda: each(p - 2, run4))

    lax.fori_loop(0, pairs, lambda p, c: (pair_step(p), c)[1], 0)
    ps_ready()
    ps_send(1, 12)
    l3_step(*tail)
    each(pairs - 2, run4)
    each(pairs - 1, run3)
    add_step(False, *tail[:3], r2t)
    ps_send(12, 22)
    each(pairs - 1, run4)
    ps_send(22, ROWS)
    s_own[0].wait()
    ps_own.wait()
    for k in range(1, RING):
        s_copy(0, k).wait_recv()
    for k in range(1, ROWS):
        ps_copy(k).wait_recv()
    l5_step(*tail, ct, TAIL)
    loop(0, lambda t: l5_step(*at(t), col0(t), CW))
    for i in range(N_CH + 1):
        o_copy(i, i * CW, CW if i < N_CH else TAIL).wait()

    for c in (g0, g1, g2, g3, a0, a1, a2, a3, b0, b1, b2, b3):
        c.wait_send()
    for rel in range(RING):
        xs = (x + rel) % RING
        for k in range(RING):
            c = t_copy(xs, (y + k) % RING)
            if k == 0:
                pl.when(xs != z)(c.wait_send)
            else:
                c.wait_send()
    v_each(lambda c: c.wait_send(), None)
    for k in range(1, PLANE):
        x_copy(k).wait_send()
    for k in range(1, RING):
        m_copy(k).wait_send()
        s_copy(0, k).wait_send()
        s_copy(1, k).wait_send()
    for k in range(1, ROWS):
        ps_copy(k).wait_send()


def sweep_call(ts, l1, l2, vs, wd, wx, v, t2, oo):
    n_p, rows, n_c = ts.shape
    n_k, n_v, n_j = wd.shape
    cols = t2.shape[1]
    k8 = rows // RING
    n_i = PLANE * rows
    blk = (RING, k8, cols)
    n = N_CH + 1
    dma = pltpu.SemaphoreType.DMA
    vm = pl.BlockSpec(memory_space=pltpu.VMEM)
    hbm = pl.BlockSpec(memory_space=pl.ANY)

    def b16(*shape):
        return pltpu.VMEM(shape, BF16)

    def f32(*shape):
        return pltpu.VMEM(shape, F32)

    def sems(*shape):
        return dma(shape)

    one, two, four, six = (), (2,), (RING,), (n, 6)
    all16, sq = (PLANE,), (RING, RING)
    v9 = (-(-cols // 640),)
    counts = [four, four, sq, all16, four, four, four, four, sq, all16, one, one, (8,), two, two, two,
              v9, v9, v9, one, one, all16, all16, four, four, six, six, six, six, (2, RING), (2, RING), (ROWS,), (ROWS,), (n,), two]
    return pl.pallas_call(
        sweep_kernel,
        out_shape=jax.ShapeDtypeStruct((rows, cols), F32),
        in_specs=[vm, vm, vm, vm, hbm, hbm, hbm, vm, hbm],
        out_specs=hbm,
        scratch_shapes=[
            b16(RING, n_p, rows, n_c), b16(2, PLANE, rows, n_c), b16(2, 2, PLANE, k8, n_c),
            b16(RING, *l1.shape), b16(RING, *l2.shape),
            b16(2, RING, n_v, n_j), b16(2, n_k // 2, FULL, n_j), b16(2, n_k, EDGE, n_j),
            f32(n_v, n_j), f32(n_v, n_j), f32(k8, n_v, n_v), f32(k8, n_v, n_v), f32(2, *blk), f32(*blk), f32(*blk), f32(rows, cols), f32(rows, cols), b16(2, k8, 2 * n_i), f32(2, k8, n_i),
            b16(2, n_c, cols), b16(2, rows, cols), b16(n_i, 2 * rows),
            f32(2, PLANE, k8, n_i), f32(PLANE, 2, k8, n_i), b16(RING, 2, k8, n_i),
            f32(N_CH, RING, RING, rows, CW), f32(RING, RING, rows, TAIL),
            f32(N_CH, 6, 2, rows, CW), f32(6, 2, rows, TAIL),
            f32(N_CH, 6, rows // 2, CW), f32(6, rows // 2, TAIL),
        ] + [sems(*c) if c else dma for c in counts],
        compiler_params=pltpu.CompilerParams(has_side_effects=True, collective_id=0, vmem_limit_bytes=VMEM_LIMIT),
        name="sweep",
    )(ts, l1, l2, vs, wd, wx, v, t2, oo)


def solution(mesh):
    n_col = mesh.shape["col"]
    amp_spec = P("row", "col")
    wide_spec = P(None, "col")

    def local_sweep(t_blk, d_blk, oovv_blk, vvvv_blk, oooo_full, wd_blk, wx_blk):
        rows_dev, cols_dev = t_blk.shape
        n_occ = math.isqrt(oooo_full.shape[0])
        n_virt = wd_blk.shape[0] // n_occ
        occ_col = n_occ // n_col
        virt_col = n_virt // n_col
        c_dev = vvvv_blk.shape[0]
        n_p = cols_dev // c_dev
        x = lax.axis_index("col")
        t_half = t_blk.astype(BF16)
        ts = t_half.reshape(rows_dev, n_p, c_dev).transpose(1, 0, 2)
        vs = oovv_blk.reshape(n_col, occ_col, n_p, c_dev).transpose(2, 0, 1, 3)
        t3 = t_half.reshape(n_occ, virt_col, n_virt)
        l1 = t3.transpose(1, 0, 2).reshape(virt_col, n_occ * n_virt)
        l1 = jnp.pad(l1, ((0, 12), (0, 0)))
        tb = t3.transpose(2, 0, 1)
        odd = x % 2 == 1
        rest = virt_col - FULL
        gap = jnp.zeros((n_virt, n_occ, EDGE - rest), BF16)
        full = jnp.where(odd, tb[:, :, rest:], tb[:, :, :FULL]).reshape(n_virt, n_occ * FULL)
        edge = jnp.where(odd, jnp.concatenate([gap, tb[:, :, :rest]], axis=2), jnp.concatenate([tb[:, :, FULL:], gap], axis=2))
        l2 = jnp.concatenate([full, edge.reshape(n_virt, n_occ * EDGE)], axis=1)
        wd3 = wd_blk.reshape(n_occ, n_virt, occ_col * n_virt)
        wx3 = wx_blk.reshape(n_occ, n_virt, occ_col * n_virt)
        summed = sweep_call(ts, l1, l2, vs, wd3, wx3, vvvv_blk, t_half, oooo_full)
        return (oovv_blk.astype(F32) + summed) / d_blk

    return jax.shard_map(local_sweep, mesh=mesh, in_specs=(amp_spec, amp_spec, amp_spec, amp_spec, P(), wide_spec, wide_spec), out_specs=amp_spec, check_vma=False)
```

```python
import math
import jax
import jax.numpy as jnp
from jax import lax
from jax.experimental import pallas as pl
from jax.experimental.pallas import tpu as pltpu
from jax.sharding import PartitionSpec as P

MESH = pl.DeviceIdType.MESH
BF16 = jnp.bfloat16
F32 = jnp.float32
VMEM_LIMIT = 67_043_328
LANE = 128
RING = 4
PLANE = 16
ROWS = 32
FULL = 32
EDGE = 8
N_CH = 10
EARLY = 5
CW = 512
TAIL = 64


def _place():
    x = lax.axis_index("col")
    r = lax.axis_index("row")
    q = r // 2
    return x, q // RING, q % RING, r % 2, q, r


def _rc(src, dst, ssem, rsem, dev):
    return pltpu.make_async_remote_copy(src_ref=src, dst_ref=dst, send_sem=ssem, recv_sem=rsem, device_id=dev, device_id_type=MESH)


def _enter(x, r):
    bar = pltpu.get_barrier_semaphore()

    def tell(dev):
        pl.semaphore_signal(bar, inc=1, device_id=dev, device_id_type=MESH)

    for k in range(1, RING):
        tell(((x + k) % RING, r))
    for k in range(1, ROWS):
        tell((x, (r + k) % ROWS))

    pl.semaphore_wait(bar, RING - 1 + ROWS - 1)


def sweep_kernel(tv, l1, l2, wd, wx, v_hbm, t2, oo_hbm, out_hbm,
                 h_in, hv, vo, tl, lg1, lg2, wdb, wxb, wxs, d_n, e_n, s_f, s_b, sw, s1_in, s2_in, ps_in, out, oo2, oo, v_buf, t_pair, m_t, x_part, x_in, m_all,
                 p_b, p_t, r1, r1t, r2, r2t,
                 g_s, g_r, h_s, h_r, t_s, t_r, p_s, p_r, o_s, o_r, f_s, f_r, loc, wd_s, wx_s, wy_s,
                 vl_s, vx_s, vx_r, tp_s, tp_r, x_s, x_r, m_s, m_r, s1, w1, s2, w2, sw_s, sw_r, ps_s, ps_r, out_s, oo_s):
    x, z, y, core, q, r = _place()
    right, left = (x + 1) % RING, (x + RING - 1) % RING
    mate = (x, q * 2 + 1 - core)
    n_kd, n_v, n_j = wd.shape
    k8, n_c = tl.shape[3:]
    rows = RING * k8
    loc_g, loc_t, loc_1, loc_2, loc_v, loc_p, loc_a, loc_b = [loc.at[i] for i in range(loc.shape[0])]
    _enter(x, r)

    def ring(src, buf, ss, rr, axis):
        h = src.shape[axis] // 2

        def part(i):
            return (pl.ds(i * h, h),) if axis == 0 else (slice(None), pl.ds(i * h, h))

        def hop(i, who, blk, to):
            ref = buf.at[(blk,) + part(i - 2)]
            return _rc(ref, ref, ss.at[i], rr.at[i], (to, who))

        c0 = _rc(src, buf.at[x], ss.at[0], rr.at[0], (right, r))
        c1 = _rc(src, buf.at[x], ss.at[1], rr.at[1], (left, r))
        return c0, c1, lambda: hop(2, r, left, right), lambda: hop(3, r, right, left)

    own1 = pltpu.make_async_copy(l1, lg1.at[x], loc_1)
    own2 = pltpu.make_async_copy(l2, lg2.at[x], loc_2)
    def h_copy(k):
        xd = (x + k) % RING
        return _rc(tv.at[xd], h_in.at[x], h_s.at[k], h_r.at[k], (xd, r))

    for k in (1, RING - 1, 2):
        h_copy(k).start()
    own1.start()
    own2.start()

    def onward(r0, r1_, f0, f1):
        r0.wait_recv()
        f0 = f0()
        f0.start()
        r1_.wait_recv()
        f1 = f1()
        f1.start()
        return [f0, f1]

    def wd_copy(i):
        return pltpu.make_async_copy(wd.at[pl.ds(RING * i, RING)], wdb.at[i % 2], wd_s.at[i % 2])

    def wx_copy(i):
        c, h = i // 2, n_kd // 2
        src = wx.at[pl.ds(i % 2 * h, h), pl.ds(FULL * c + EDGE * ((c + 1) // 2), FULL)]
        return pltpu.make_async_copy(src, wxb.at[i % 2], wx_s.at[i % 2])

    def wy_copy(i):
        return pltpu.make_async_copy(wx.at[:, pl.ds(FULL + n_v // 2 * i, EDGE)], wxs.at[i], wy_s.at[i])

    def oo_copy(i):
        k0 = pl.multiple_of((2 * q + i) * rows + x * EDGE, EDGE)
        return pltpu.make_async_copy(oo_hbm.at[pl.ds(k0, EDGE)], oo2.at[i], oo_s.at[i])

    for i in range(2):
        oo_copy(i).start()
        wd_copy(i).start()
        wx_copy(i).start()
        wy_copy(i).start()

    def piece(xs, yd, buf):
        return buf.at[xs, pl.ds(2 * yd, 2)]

    def t_copy(xs, yd, buf):
        return _rc(piece(xs, yd, buf), hv.at[:, :, q], t_s, t_r, (x, (xs * RING + yd) * 2 + core))

    def t_own(xs, buf):
        return pltpu.make_async_copy(piece(xs, y, buf), hv.at[:, :, q], loc_t)

    def t_block(rel):
        xs = (x + rel) % RING
        buf = tv if rel == 0 else h_in
        for k in range(RING):
            yd = (y + k) % RING
            if k == 0:
                pl.when(xs == z)(lambda: t_own(xs, buf).start())
                pl.when(xs != z)(lambda: t_copy(xs, yd, buf).start())
            else:
                t_copy(xs, yd, buf).start()

    t_block(0)
    a0, a1, a2, a3 = ring(l1, lg1, p_s, p_r, 1)
    b0, b1, b2, b3 = ring(l2, lg2, o_s, o_r, 1)
    a0.start()
    a1.start()
    for k in (1, RING - 1, 2):
        h_copy(k).wait_recv()
        t_block(RING - k)

    n_v9 = vl_s.shape[0]
    wide = 640
    v_in = []
    for i in range(n_v9):
        c0 = i * wide
        w = min(wide, v_hbm.shape[1] - c0)
        src, dst = v_hbm.at[:, pl.ds(c0, w)], v_buf.at[core, :, pl.ds(c0, w)]
        v_in += [pltpu.make_async_copy(src, dst, vl_s.at[i]), _rc(src, dst, vx_s.at[i], vx_r.at[i], mate)]
    v_in += [pltpu.make_async_copy(t2, t_pair.at[core], loc_p), _rc(t2, t_pair.at[core], tp_s, tp_r, mate)]
    for c in v_in:
        c.start()

    for i in range(2):
        oo_copy(i).wait()
    ow = oo2[...].astype(F32)
    for k in range(PLANE):
        c0 = 2 * k * rows
        oo[:, :, k * rows:(k + 1) * rows] = jnp.where(core == 1, ow[:, :, c0 + rows:c0 + 2 * rows], ow[:, :, c0:c0 + rows])
    ot = oo[...].reshape(2 * k8, PLANE * rows).T
    ot = jnp.concatenate([ot[k * rows + i * k8:k * rows + (i + 1) * k8] for i in range(RING) for k in range(PLANE)], axis=0)
    oo[...] = ot.T.reshape(2, k8, PLANE * rows)

    t_own(x, tv).wait()
    t_others = hv.at[:, :, pl.ds(0, PLANE - 1)]
    pltpu.make_async_copy(t_others, t_others, t_r).wait()
    g0, g1, g2, g3 = ring(hv.at[:, 0], tl, g_s, g_r, 0)
    g0.start()
    g1.start()
    fwd = _rc(hv.at[:, 1], vo, f_s, f_r, mate)
    fwd.start()
    own = pltpu.make_async_copy(hv.at[:, 0], tl.at[x], loc_g)
    own.start()
    g0.wait_recv()
    g2 = g2()
    g2.start()
    g1.wait_recv()
    g3 = g3()
    g3.start()
    a_fwd = onward(a0, a1, a2, a3)
    fwd.wait()
    own.wait()
    g2.wait_recv()
    g3.wait_recv()

    n_i = PLANE * rows
    n_k = PLANE * k8
    dn = (((1,), (1,)), ((), ()))

    def x_of(v_mine, v_ref):
        acc = None
        for i in range(2):
            v_i = (v_ref[i, 1] if v_mine else v_ref[i]).reshape(n_k, n_c)
            d = lax.dot_general(v_i, tl[:, i].reshape(n_i, n_c), dn, preferred_element_type=F32)
            acc = d if acc is None else acc + d
        return acc.reshape(PLANE, k8, n_i)

    x_part[core] = x_of(True, hv)
    x_part[1 - core] = x_of(False, vo)

    def x_copy(k):
        qd = (q + k) % PLANE
        return _rc(x_part.at[:, qd], x_in.at[q], x_s, x_r, (x, qd * 2 + core))

    for k in range(1, PLANE):
        x_copy(k).start()
    x_in[q] = x_part[:, q]
    others = x_in.at[pl.ds(0, PLANE - 1)]
    pltpu.make_async_copy(others, others, x_r).wait()
    xs = x_in[0]
    for k in range(1, PLANE):
        xs = xs + x_in[k]
    m_all[x] = (oo[...] + 0.5 * xs).astype(BF16)

    def m_copy(k):
        return _rc(m_all.at[x], m_all.at[x], m_s.at[k], m_r.at[k], ((x + k) % RING, r))

    for k in range(1, RING):
        m_copy(k).start()
    b0.start()
    b1.start()

    def s_copy(i, k):
        xd = (x + k) % RING
        return _rc(sw.at[i, xd], (s1_in, s2_in)[i].at[x], sw_s.at[i, k], sw_r.at[i, k], (xd, r))

    s_own = [pltpu.make_async_copy(sw.at[i, x], (s1_in, s2_in)[i].at[x], (loc_a, loc_b)[i]) for i in range(2)]
    def ps_src(rd):
        return s2_in.at[rd // EDGE, pl.ds(rd % EDGE, 1)]

    def ps_copy(k):
        rd = (r + k) % ROWS
        return _rc(ps_src(rd), ps_in.at[pl.ds(r, 1)], ps_s.at[k], ps_r.at[k], (x, rd))

    ps_own = pltpu.make_async_copy(ps_src(r), ps_in.at[pl.ds(r, 1)], loc_g)

    def ps_ready():
        s_own[1].wait()
        for k in range(1, RING):
            s_copy(1, k).wait_recv()
        ps_own.start()

    def ps_send(lo, hi):
        for k in range(lo, hi):
            ps_copy(k).start()

    n1 = l1.shape[0]
    quarter = n_v // RING

    def r3_work(a_fwd):
        own1.wait()
        own2.wait()
        for c in a_fwd:
            c.wait_recv()
        acc = None
        kd = RING * n_v
        for i in range(2 * RING):
            wd_copy(i).wait()
            lhs = lg1[:, :, i * kd:(i + 1) * kd].reshape(RING * n1, kd)
            d = jnp.dot(lhs, wdb[i % 2].reshape(kd, n_j), preferred_element_type=F32)
            acc = d if acc is None else acc + d
            if i + 2 < 2 * RING:
                wd_copy(i + 2).start()
        for i in range(RING):
            d_n[quarter * i:quarter * (i + 1), :] = acc[n1 * i:n1 * i + quarter]

    def r5_work(b_fwd):
        for c in b_fwd:
            c.wait_recv()
        acc = None
        kb = FULL * n_kd
        kh = kb // 2
        for i in range(2 * RING):
            wx_copy(i).wait()
            d = jnp.dot(lg2[i // 2, :, i % 2 * kh:(i % 2 + 1) * kh], wxb[i % 2].reshape(kh, n_j), preferred_element_type=F32)
            acc = d if acc is None else acc + d
            if i + 2 < 2 * RING:
                wx_copy(i + 2).start()
        for i in range(2):
            wy_copy(i).wait()
            lhs = lg2[2 * i, :, kb:] + lg2[2 * i + 1, :, kb:]
            acc = acc + jnp.dot(lhs, wxs[i].reshape(EDGE * n_kd, n_j), preferred_element_type=F32)
        e_n[...] = acc

        for j in range(n_j // n_v):
            cut = slice(j * n_v, (j + 1) * n_v)
            sj = d_n[:, cut] - e_n[:, cut].T
            s_f[j] = sj
            s_b[j] = sj.T
        for i in range(2):
            for a in range(n_v):
                c0 = a % quarter * n_v
                sw[i, a // quarter, :, c0:c0 + n_v] = (s_f, s_b)[i][:, a, :]
        for i in (1, 0):
            for k in range(1, RING):
                s_copy(i, k).start()
            s_own[i].start()


    for c in v_in:
        c.wait()
    for k in range(1, RING):
        m_copy(k).wait_recv()
    mf = m_all[...].astype(F32)
    m_t[...] = jnp.concatenate([mf[xx, cc] for cc in range(2) for xx in range(RING)], axis=0).T.astype(BF16)

    def to(first, a, d):
        b = a if first else 1 - a
        return (x, (((z + d * (1 - b)) % RING) * RING + (y + d * b) % RING) * 2 + core)

    def coords(a):
        return y * a + z * (1 - a), z * a + y * (1 - a)

    def stage(first, t, a, pb, rb):
        u, v = coords(a)
        c, pre, n = (u, (), 2) if first else (v, (u,), rows // 2)
        lo, hi = pl.ds(0, n), pl.ds(n, n)
        far, up, dn_ = (c + 2) % RING, (c + 1) % RING, (c + RING - 1) % RING
        ss, ww = (s1, w1) if first else (s2, w2)
        last = isinstance(t, int) and t == N_CH
        srcs = (far, lo), (far, hi), (up, hi), (dn_, lo), (up, lo), (dn_, hi)

        def msg(i):
            d = 1 if i % 2 == 0 else RING - 1
            return _rc(pb.at[pre + srcs[i]], rb.at[i], ss.at[int(last)], ww.at[t, min(i, 2)], to(first, a, d))
        return msg

    def near(rb, ww, t):
        got = rb.at[pl.ds(2, 4)]
        pltpu.make_async_copy(got, got, ww.at[t, 2]).wait()

    def l1_step(t, a, pb, rb, c0, w):
        tp = t_pair[:, :, pl.ds(c0, w)].reshape(2 * rows, w)
        acc = jnp.dot(m_t[...], tp, preferred_element_type=F32)
        for i in range(2):
            acc = acc + jnp.dot(tl[:, i].reshape(n_i, n_c), v_buf[i, :, pl.ds(c0, w)], preferred_element_type=F32)
        for zb in range(RING):
            for yb in range(RING):
                for i in range(RING):
                    b = i * n_k + (zb * RING + yb) * k8
                    pb[yb * a + zb * (1 - a), zb * a + yb * (1 - a), i * k8:(i + 1) * k8] = acc[b:b + k8]
        msg = stage(True, t, a, pb, rb)
        msg(0).start()
        msg(1).start()

    def plain_step(t, a, pb, rb):
        msg = stage(True, t, a, pb, rb)
        msg(2).start()
        msg(3).start()

    def add_step(first, t, a, pb, rb):
        u, v = coords(a)
        c, pre, n = (u, (), 2) if first else (v, (u,), rows // 2)
        msg = stage(first, t, a, pb, rb)
        msg(0).wait_recv()
        up = pre + ((c + 1) % RING, pl.ds(0, n))
        pb[up] = pb[up] + rb[0]
        msg(4).start()
        msg(1).wait_recv()
        dn_ = pre + ((c + RING - 1) % RING, pl.ds(n, n))
        pb[dn_] = pb[dn_] + rb[1]
        msg(5).start()

    def l3_step(t, a, pb, rb, rb2):
        u, _ = coords(a)
        near(rb, w1, t)
        pb[u, :2] = pb[u, :2] + rb[4] + rb[3]
        pb[u, 2:] = pb[u, 2:] + rb[2] + rb[5]
        nxt = stage(False, t, a, pb, rb2)
        for i in range(4):
            nxt(i).start()

    def o_copy(t, c0, w):
        return pltpu.make_async_copy(out.at[:, pl.ds(c0, w)], out_hbm.at[:, pl.ds(c0, w)], out_s.at[t])

    def l5_step(t, a, pb, rb, rb2, c0, w):
        u, v = coords(a)
        h = rows // 2
        near(rb2, w2, t)
        sym = s1_in[:, :, pl.ds(c0, w)].reshape(rows, w) + ps_in[:, pl.ds(c0, w)]
        out[:h, pl.ds(c0, w)] = pb[u, v, :h] + rb2[4] + rb2[3] + sym[:h]
        out[h:, pl.ds(c0, w)] = pb[u, v, h:] + rb2[2] + rb2[5] + sym[h:]
        o_copy(t, c0, w).start()

    def at(t):
        return (t, 1 - t % 2, p_b.at[t], r1.at[t], r2.at[t])

    def col0(t):
        return pl.multiple_of((t // 2) * CW + (t % 2) * (N_CH // 2) * CW, LANE)

    def loop(lo, fn, hi=N_CH):
        lax.fori_loop(lo, hi, lambda t, c: (fn(t), c)[1], 0)

    tail = (N_CH, 1, p_t, r1t, r2t)
    ct = N_CH * CW

    def run1(t):
        n, a, pb, rb, _ = at(t)
        l1_step(n, a, pb, rb, col0(t), CW)

    def run2(t):
        add_step(True, *at(t)[:4])

    def run3(t):
        l3_step(*at(t))

    def run4(t):
        n, a, pb, _, rb2 = at(t)
        add_step(False, n, a, pb, rb2)

    loop(0, run1, EARLY)
    b_fwd = onward(b0, b1, b2, b3)
    loop(EARLY, run1)
    l1_step(*tail[:4], ct, TAIL)
    loop(0, lambda t: plain_step(*at(t)[:4]))
    plain_step(*tail[:4])
    r3_work(a_fwd)
    loop(0, run2)
    add_step(True, *tail[:4])
    r5_work(b_fwd)
    loop(0, run3, EARLY + 1)
    ps_ready()
    ps_send(1, ROWS)
    loop(EARLY + 1, run3)
    l3_step(*tail)
    loop(0, run4, EARLY + 1)
    loop(EARLY + 1, run4)
    add_step(False, *tail[:3], r2t)
    s_own[0].wait()
    ps_own.wait()
    for k in range(1, RING):
        s_copy(0, k).wait_recv()
    for k in range(1, ROWS):
        ps_copy(k).wait_recv()
    l5_step(*tail, ct, TAIL)
    loop(0, lambda t: l5_step(*at(t), col0(t), CW))
    for i in range(N_CH + 1):
        o_copy(i, i * CW, CW if i < N_CH else TAIL).wait()

    for sem, bufs in ((s1, (r1, r1t)), (s2, (r2, r2t))):
        for i in range(2):
            pltpu.make_async_copy(bufs[i], bufs[i], sem.at[i]).wait()
    for c in (g0, g1, g2, g3, a0, a1, b0, b1, *a_fwd, *b_fwd):
        c.wait_send()
    pltpu.make_async_copy(t_others, t_others, t_s).wait()
    for k in range(1, RING):
        h_copy(k).wait_send()
    pltpu.make_async_copy(others, others, x_s).wait()
    for k in range(1, RING):
        m_copy(k).wait_send()
        s_copy(0, k).wait_send()
        s_copy(1, k).wait_send()
    for k in range(1, ROWS):
        ps_copy(k).wait_send()


def sweep_call(tv, l1, l2, wd, wx, v, t2, oo):
    n_p, n_c = tv.shape[1], tv.shape[4]
    rows = t2.shape[0]
    n_k, n_v, n_j = wd.shape
    cols = t2.shape[1]
    k8 = rows // RING
    n_i = PLANE * rows
    blk = (RING, k8, cols)
    n = N_CH + 1
    dma = pltpu.SemaphoreType.DMA
    vm = pl.BlockSpec(memory_space=pltpu.VMEM)
    hbm = pl.BlockSpec(memory_space=pl.ANY)

    def b16(*shape):
        return pltpu.VMEM(shape, BF16)

    def f32(*shape):
        return pltpu.VMEM(shape, F32)

    def sems(*shape):
        return dma(shape)

    one, two, four, six = (), (2,), (RING,), (n, 3)
    v9 = (-(-cols // 640),)
    counts = [four, four, four, four, one, one, four, four, four, four, one, one, (8,), two, two, two,
              v9, v9, v9, one, one, one, one, four, four, two, six, two, six, (2, RING), (2, RING), (ROWS,), (ROWS,), (n,), two]
    return pl.pallas_call(
        sweep_kernel,
        out_shape=jax.ShapeDtypeStruct((rows, cols), F32),
        in_specs=[vm, vm, vm, hbm, hbm, hbm, vm, hbm],
        out_specs=hbm,
        scratch_shapes=[
            b16(*tv.shape), b16(2, 2, PLANE, k8, n_c), b16(2, PLANE, k8, n_c), b16(RING, 2, PLANE, k8, n_c),
            b16(RING, *l1.shape), b16(RING, *l2.shape),
            b16(2, RING, n_v, n_j), b16(2, n_k // 2, FULL, n_j), b16(2, n_k, EDGE, n_j),
            f32(n_v, n_j), f32(n_v, n_j), f32(k8, n_v, n_v), f32(k8, n_v, n_v), f32(2, *blk), f32(*blk), f32(*blk), f32(rows, cols), f32(rows, cols), b16(2, k8, 2 * n_i), f32(2, k8, n_i),
            b16(2, n_c, cols), b16(2, rows, cols), b16(n_i, 2 * rows),
            f32(2, PLANE, k8, n_i), f32(PLANE, 2, k8, n_i), b16(RING, 2, k8, n_i),
            f32(N_CH, RING, RING, rows, CW), f32(RING, RING, rows, TAIL),
            f32(N_CH, 6, 2, rows, CW), f32(6, 2, rows, TAIL),
            f32(N_CH, 6, rows // 2, CW), f32(6, rows // 2, TAIL),
        ] + [sems(*c) if c else dma for c in counts],
        compiler_params=pltpu.CompilerParams(has_side_effects=True, collective_id=0, vmem_limit_bytes=VMEM_LIMIT),
        name="sweep",
    )(tv, l1, l2, wd, wx, v, t2, oo)


def solution(mesh):
    n_col = mesh.shape["col"]
    amp_spec = P("row", "col")
    wide_spec = P(None, "col")

    def local_sweep(t_blk, d_blk, oovv_blk, vvvv_blk, oooo_full, wd_blk, wx_blk):
        rows_dev, cols_dev = t_blk.shape
        n_occ = math.isqrt(oooo_full.shape[0])
        n_virt = wd_blk.shape[0] // n_occ
        occ_col = n_occ // n_col
        virt_col = n_virt // n_col
        c_dev = vvvv_blk.shape[0]
        n_p = cols_dev // c_dev
        x = lax.axis_index("col")
        t_half = t_blk.astype(BF16)
        tv = jnp.stack([a.reshape(n_col, occ_col, n_p, c_dev).transpose(0, 2, 1, 3) for a in (t_half, oovv_blk)], axis=2)
        t3 = t_half.reshape(n_occ, virt_col, n_virt)
        l1 = t3.transpose(1, 0, 2).reshape(virt_col, n_occ * n_virt)
        l1 = jnp.pad(l1, ((0, 12), (0, 0)))
        tb = t3.transpose(2, 0, 1)
        odd = x % 2 == 1
        rest = virt_col - FULL
        gap = jnp.zeros((n_virt, n_occ, EDGE - rest), BF16)
        full = jnp.where(odd, tb[:, :, rest:], tb[:, :, :FULL]).reshape(n_virt, n_occ * FULL)
        edge = jnp.where(odd, jnp.concatenate([gap, tb[:, :, :rest]], axis=2), jnp.concatenate([tb[:, :, FULL:], gap], axis=2))
        l2 = jnp.concatenate([full, edge.reshape(n_virt, n_occ * EDGE)], axis=1)
        wd3 = wd_blk.reshape(n_occ, n_virt, occ_col * n_virt)
        wx3 = wx_blk.reshape(n_occ, n_virt, occ_col * n_virt)
        summed = sweep_call(tv, l1, l2, wd3, wx3, vvvv_blk, t_half, oooo_full)
        return (oovv_blk.astype(F32) + summed) / d_blk

    return jax.shard_map(local_sweep, mesh=mesh, in_specs=(amp_spec, amp_spec, amp_spec, amp_spec, P(), wide_spec, wide_spec), out_specs=amp_spec, check_vma=False)
```

```python
import math
import jax
import jax.numpy as jnp
from jax import lax
from jax.experimental import pallas as pl
from jax.experimental.pallas import tpu as pltpu
from jax.sharding import PartitionSpec as P

MESH = pl.DeviceIdType.MESH
BF16 = jnp.bfloat16
F32 = jnp.float32
VMEM_LIMIT = 67_043_328
LANE = 128
RING = 4
PLANE = 16
ROWS = 32
FULL = 32
EDGE = 8
N_CH = 10
EARLY = 5
CW = 512
TAIL = 64


def _place():
    x = lax.axis_index("col")
    r = lax.axis_index("row")
    q = r // 2
    return x, q // RING, q % RING, r % 2, q, r


def _rc(src, dst, ssem, rsem, dev):
    return pltpu.make_async_remote_copy(src_ref=src, dst_ref=dst, send_sem=ssem, recv_sem=rsem, device_id=dev, device_id_type=MESH)


def _enter(x, r):
    bar = pltpu.get_barrier_semaphore()

    def tell(dev):
        pl.semaphore_signal(bar, inc=1, device_id=dev, device_id_type=MESH)

    for k in range(1, RING):
        tell(((x + k) % RING, r))
    for k in range(1, ROWS):
        tell((x, (r + k) % ROWS))

    pl.semaphore_wait(bar, RING - 1 + ROWS - 1)


def sweep_kernel(t_in, ov_in, wd, wx, v_hbm, oo_hbm, out_hbm,
                 tv, l1, l2, t2,
                 h_in, hv, vo, tl, lg1, lg2, wdb, wxb, wxs, d_n, e_n, s_f, s_b, sw, s1_in, s2_in, ps_in, out, oo2, oo, v_buf, t_pair, m_t, x_part, x_in, m_all,
                 p_b, p_t, r1, r1t, r2, r2t,
                 g_s, g_r, h_s, h_r, t_s, t_r, p_s, p_r, o_s, o_r, f_s, f_r, loc, wd_s, wx_s, wy_s,
                 vl_s, vx_s, vx_r, tp_s, tp_r, x_s, x_r, m_s, m_r, s1, w1, s2, w2, sw_s, sw_r, ps_s, ps_r, out_s, oo_s):
    x, z, y, core, q, r = _place()
    right, left = (x + 1) % RING, (x + RING - 1) % RING
    mate = (x, q * 2 + 1 - core)
    n_kd, n_v, n_j = wd.shape
    k8, n_c = tl.shape[3:]
    rows = RING * k8
    loc_g, loc_t, loc_1, loc_2, loc_v, loc_p, loc_a, loc_b = [loc.at[i] for i in range(loc.shape[0])]

    t2[...] = t_in[...].astype(BF16)
    for xd in range(RING):
        rq = slice(xd * k8, (xd + 1) * k8)
        for i, val in enumerate((t_in[rq, :], ov_in[rq, :].astype(F32))):
            for p in range(tv.shape[1]):
                tv[xd, p, i] = val[:, p * n_c:(p + 1) * n_c].astype(BF16)
    _enter(x, r)

    def ring(src, buf, ss, rr, axis):
        h = src.shape[axis] // 2

        def part(i):
            return (pl.ds(i * h, h),) if axis == 0 else (slice(None), pl.ds(i * h, h))

        def hop(i, who, blk, to):
            ref = buf.at[(blk,) + part(i - 2)]
            return _rc(ref, ref, ss.at[i], rr.at[i], (to, who))

        c0 = _rc(src, buf.at[x], ss.at[0], rr.at[0], (right, r))
        c1 = _rc(src, buf.at[x], ss.at[1], rr.at[1], (left, r))
        return c0, c1, lambda: hop(2, r, left, right), lambda: hop(3, r, right, left)

    own1 = pltpu.make_async_copy(l1, lg1.at[x], loc_1)
    own2 = pltpu.make_async_copy(l2, lg2.at[x], loc_2)
    def h_copy(k):
        xd = (x + k) % RING
        return _rc(tv.at[xd], h_in.at[x], h_s.at[k], h_r.at[k], (xd, r))

    for k in (1, RING - 1, 2):
        h_copy(k).start()

    def onward(r0, r1_, f0, f1):
        r0.wait_recv()
        f0 = f0()
        f0.start()
        r1_.wait_recv()
        f1 = f1()
        f1.start()
        return [f0, f1]

    def wd_copy(i):
        return pltpu.make_async_copy(wd.at[pl.ds(RING * i, RING)], wdb.at[i % 2], wd_s.at[i % 2])

    def wx_copy(i):
        c, h = i // 2, n_kd // 2
        src = wx.at[pl.ds(i % 2 * h, h), pl.ds(FULL * c + EDGE * ((c + 1) // 2), FULL)]
        return pltpu.make_async_copy(src, wxb.at[i % 2], wx_s.at[i % 2])

    def wy_copy(i):
        return pltpu.make_async_copy(wx.at[:, pl.ds(FULL + n_v // 2 * i, EDGE)], wxs.at[i], wy_s.at[i])

    def oo_copy(i):
        k0 = pl.multiple_of((2 * q + i) * rows + x * EDGE, EDGE)
        return pltpu.make_async_copy(oo_hbm.at[pl.ds(k0, EDGE)], oo2.at[i], oo_s.at[i])

    for i in range(2):
        oo_copy(i).start()
        wd_copy(i).start()
        wx_copy(i).start()
        wy_copy(i).start()

    def piece(xs, yd, buf):
        return buf.at[xs, pl.ds(2 * yd, 2)]

    def t_copy(xs, yd, buf):
        return _rc(piece(xs, yd, buf), hv.at[:, :, q], t_s, t_r, (x, (xs * RING + yd) * 2 + core))

    def t_own(xs, buf):
        return pltpu.make_async_copy(piece(xs, y, buf), hv.at[:, :, q], loc_t)

    def t_block(rel):
        xs = (x + rel) % RING
        buf = tv if rel == 0 else h_in
        for k in range(RING):
            yd = (y + k) % RING
            if k == 0:
                pl.when(xs == z)(lambda: t_own(xs, buf).start())
                pl.when(xs != z)(lambda: t_copy(xs, yd, buf).start())
            else:
                t_copy(xs, yd, buf).start()

    t_block(0)
    quarter = n_v // RING
    groups = t2.shape[0] // EDGE
    for a in range(quarter):
        for kk in range(groups):
            s_f[:, quarter * kk + a, :] = t_in[EDGE * kk:EDGE * (kk + 1), n_v * a:n_v * (a + 1)]
    rest = quarter - FULL
    odd = x % 2 == 1
    none = jnp.zeros((n_v, EDGE - rest), F32)
    for k in range(t2.shape[0]):
        kk = k // EDGE
        bt = s_f[k % EDGE, quarter * kk:quarter * (kk + 1), :].T
        e_n[:, FULL * k:FULL * (k + 1)] = jnp.where(odd, bt[:, rest:], bt[:, :FULL])
        d_n[:, EDGE * k:EDGE * (k + 1)] = jnp.where(odd, jnp.concatenate([none, bt[:, :rest]], axis=1), jnp.concatenate([bt[:, FULL:], none], axis=1))
    l2[:, :FULL * n_kd] = e_n[:, :FULL * n_kd].astype(BF16)
    l2[:, FULL * n_kd:] = d_n[:, :EDGE * n_kd].astype(BF16)
    pad1 = l1.shape[0]
    d_n[:pad1, :] = jnp.zeros((pad1, n_j), F32)
    for kk in range(groups):
        for i in range(EDGE):
            d_n[:quarter, n_v * i:n_v * (i + 1)] = s_f[i, quarter * kk:quarter * (kk + 1), :]
        l1[:, n_j * kk:n_j * (kk + 1)] = d_n[:pad1, :].astype(BF16)
    own1.start()
    own2.start()
    a0, a1, a2, a3 = ring(l1, lg1, p_s, p_r, 1)
    b0, b1, b2, b3 = ring(l2, lg2, o_s, o_r, 1)
    a0.start()
    a1.start()
    for k in (1, RING - 1, 2):
        h_copy(k).wait_recv()
        t_block(RING - k)

    n_v9 = vl_s.shape[0]
    wide = 640
    v_in = []
    for i in range(n_v9):
        c0 = i * wide
        w = min(wide, v_hbm.shape[1] - c0)
        src, dst = v_hbm.at[:, pl.ds(c0, w)], v_buf.at[core, :, pl.ds(c0, w)]
        v_in += [pltpu.make_async_copy(src, dst, vl_s.at[i]), _rc(src, dst, vx_s.at[i], vx_r.at[i], mate)]
    v_in += [pltpu.make_async_copy(t2, t_pair.at[core], loc_p), _rc(t2, t_pair.at[core], tp_s, tp_r, mate)]
    for c in v_in:
        c.start()

    for i in range(2):
        oo_copy(i).wait()
    ow = oo2[...].astype(F32)
    for k in range(PLANE):
        c0 = 2 * k * rows
        oo[:, :, k * rows:(k + 1) * rows] = jnp.where(core == 1, ow[:, :, c0 + rows:c0 + 2 * rows], ow[:, :, c0:c0 + rows])
    ot = oo[...].reshape(2 * k8, PLANE * rows).T
    ot = jnp.concatenate([ot[k * rows + i * k8:k * rows + (i + 1) * k8] for i in range(RING) for k in range(PLANE)], axis=0)
    oo[...] = ot.T.reshape(2, k8, PLANE * rows)

    t_own(x, tv).wait()
    t_others = hv.at[:, :, pl.ds(0, PLANE - 1)]
    pltpu.make_async_copy(t_others, t_others, t_r).wait()
    g0, g1, g2, g3 = ring(hv.at[:, 0], tl, g_s, g_r, 0)
    g0.start()
    g1.start()
    fwd = _rc(hv.at[:, 1], vo, f_s, f_r, mate)
    fwd.start()
    own = pltpu.make_async_copy(hv.at[:, 0], tl.at[x], loc_g)
    own.start()
    g0.wait_recv()
    g2 = g2()
    g2.start()
    g1.wait_recv()
    g3 = g3()
    g3.start()
    a_fwd = onward(a0, a1, a2, a3)
    fwd.wait()
    own.wait()
    g2.wait_recv()
    g3.wait_recv()

    n_i = PLANE * rows
    n_k = PLANE * k8
    dn = (((1,), (1,)), ((), ()))

    def x_of(v_mine, v_ref):
        acc = None
        for i in range(2):
            v_i = (v_ref[i, 1] if v_mine else v_ref[i]).reshape(n_k, n_c)
            d = lax.dot_general(v_i, tl[:, i].reshape(n_i, n_c), dn, preferred_element_type=F32)
            acc = d if acc is None else acc + d
        return acc.reshape(PLANE, k8, n_i)

    x_part[core] = x_of(True, hv)
    x_part[1 - core] = x_of(False, vo)

    def x_copy(k):
        qd = (q + k) % PLANE
        return _rc(x_part.at[:, qd], x_in.at[q], x_s, x_r, (x, qd * 2 + core))

    for k in range(1, PLANE):
        x_copy(k).start()
    x_in[q] = x_part[:, q]
    others = x_in.at[pl.ds(0, PLANE - 1)]
    pltpu.make_async_copy(others, others, x_r).wait()
    xs = x_in[0]
    for k in range(1, PLANE):
        xs = xs + x_in[k]
    m_all[x] = (oo[...] + 0.5 * xs).astype(BF16)

    def m_copy(k):
        return _rc(m_all.at[x], m_all.at[x], m_s.at[k], m_r.at[k], ((x + k) % RING, r))

    for k in range(1, RING):
        m_copy(k).start()
    b0.start()
    b1.start()

    def s_copy(i, k):
        xd = (x + k) % RING
        return _rc(sw.at[i, xd], (s1_in, s2_in)[i].at[x], sw_s.at[i, k], sw_r.at[i, k], (xd, r))

    s_own = [pltpu.make_async_copy(sw.at[i, x], (s1_in, s2_in)[i].at[x], (loc_a, loc_b)[i]) for i in range(2)]
    def ps_src(rd):
        return s2_in.at[rd // EDGE, pl.ds(rd % EDGE, 1)]

    def ps_copy(k):
        rd = (r + k) % ROWS
        return _rc(ps_src(rd), ps_in.at[pl.ds(r, 1)], ps_s.at[k], ps_r.at[k], (x, rd))

    ps_own = pltpu.make_async_copy(ps_src(r), ps_in.at[pl.ds(r, 1)], loc_g)

    def ps_ready():
        s_own[1].wait()
        for k in range(1, RING):
            s_copy(1, k).wait_recv()
        ps_own.start()

    def ps_send(lo, hi):
        for k in range(lo, hi):
            ps_copy(k).start()

    n1 = l1.shape[0]

    def r3_work(a_fwd):
        own1.wait()
        own2.wait()
        for c in a_fwd:
            c.wait_recv()
        acc = None
        kd = RING * n_v
        for i in range(2 * RING):
            wd_copy(i).wait()
            lhs = lg1[:, :, i * kd:(i + 1) * kd].reshape(RING * n1, kd)
            d = jnp.dot(lhs, wdb[i % 2].reshape(kd, n_j), preferred_element_type=F32)
            acc = d if acc is None else acc + d
            if i + 2 < 2 * RING:
                wd_copy(i + 2).start()
        for i in range(RING):
            d_n[quarter * i:quarter * (i + 1), :] = acc[n1 * i:n1 * i + quarter]

    def r5_work(b_fwd):
        for c in b_fwd:
            c.wait_recv()
        acc = None
        kb = FULL * n_kd
        kh = kb // 2
        for i in range(2 * RING):
            wx_copy(i).wait()
            d = jnp.dot(lg2[i // 2, :, i % 2 * kh:(i % 2 + 1) * kh], wxb[i % 2].reshape(kh, n_j), preferred_element_type=F32)
            acc = d if acc is None else acc + d
            if i + 2 < 2 * RING:
                wx_copy(i + 2).start()
        for i in range(2):
            wy_copy(i).wait()
            lhs = lg2[2 * i, :, kb:] + lg2[2 * i + 1, :, kb:]
            acc = acc + jnp.dot(lhs, wxs[i].reshape(EDGE * n_kd, n_j), preferred_element_type=F32)
        e_n[...] = acc

        for j in range(n_j // n_v):
            cut = slice(j * n_v, (j + 1) * n_v)
            sj = d_n[:, cut] - e_n[:, cut].T
            s_f[j] = sj
            s_b[j] = sj.T
        for i in range(2):
            for a in range(n_v):
                c0 = a % quarter * n_v
                sw[i, a // quarter, :, c0:c0 + n_v] = (s_f, s_b)[i][:, a, :]
        for i in (1, 0):
            for k in range(1, RING):
                s_copy(i, k).start()
            s_own[i].start()


    for c in v_in:
        c.wait()
    for k in range(1, RING):
        m_copy(k).wait_recv()
    mf = m_all[...].astype(F32)
    m_t[...] = jnp.concatenate([mf[xx, cc] for cc in range(2) for xx in range(RING)], axis=0).T.astype(BF16)

    def to(first, a, d):
        b = a if first else 1 - a
        return (x, (((z + d * (1 - b)) % RING) * RING + (y + d * b) % RING) * 2 + core)

    def coords(a):
        return y * a + z * (1 - a), z * a + y * (1 - a)

    def stage(first, t, a, pb, rb):
        u, v = coords(a)
        c, pre, n = (u, (), 2) if first else (v, (u,), rows // 2)
        lo, hi = pl.ds(0, n), pl.ds(n, n)
        far, up, dn_ = (c + 2) % RING, (c + 1) % RING, (c + RING - 1) % RING
        ss, ww = (s1, w1) if first else (s2, w2)
        last = isinstance(t, int) and t == N_CH
        srcs = (far, lo), (far, hi), (up, hi), (dn_, lo), (up, lo), (dn_, hi)

        def msg(i):
            d = 1 if i % 2 == 0 else RING - 1
            return _rc(pb.at[pre + srcs[i]], rb.at[i], ss.at[int(last)], ww.at[t, min(i, 2)], to(first, a, d))
        return msg

    def near(rb, ww, t):
        got = rb.at[pl.ds(2, 4)]
        pltpu.make_async_copy(got, got, ww.at[t, 2]).wait()

    def l1_step(t, a, pb, rb, c0, w):
        tp = t_pair[:, :, pl.ds(c0, w)].reshape(2 * rows, w)
        acc = jnp.dot(m_t[...], tp, preferred_element_type=F32)
        for i in range(2):
            acc = acc + jnp.dot(tl[:, i].reshape(n_i, n_c), v_buf[i, :, pl.ds(c0, w)], preferred_element_type=F32)
        for zb in range(RING):
            for yb in range(RING):
                for i in range(RING):
                    b = i * n_k + (zb * RING + yb) * k8
                    pb[yb * a + zb * (1 - a), zb * a + yb * (1 - a), i * k8:(i + 1) * k8] = acc[b:b + k8]
        msg = stage(True, t, a, pb, rb)
        msg(0).start()
        msg(1).start()

    def plain_step(t, a, pb, rb):
        msg = stage(True, t, a, pb, rb)
        msg(2).start()
        msg(3).start()

    def add_step(first, t, a, pb, rb):
        u, v = coords(a)
        c, pre, n = (u, (), 2) if first else (v, (u,), rows // 2)
        msg = stage(first, t, a, pb, rb)
        msg(0).wait_recv()
        up = pre + ((c + 1) % RING, pl.ds(0, n))
        pb[up] = pb[up] + rb[0]
        msg(4).start()
        msg(1).wait_recv()
        dn_ = pre + ((c + RING - 1) % RING, pl.ds(n, n))
        pb[dn_] = pb[dn_] + rb[1]
        msg(5).start()

    def l3_step(t, a, pb, rb, rb2):
        u, _ = coords(a)
        near(rb, w1, t)
        pb[u, :2] = pb[u, :2] + rb[4] + rb[3]
        pb[u, 2:] = pb[u, 2:] + rb[2] + rb[5]
        nxt = stage(False, t, a, pb, rb2)
        for i in range(4):
            nxt(i).start()

    def o_copy(t, c0, w):
        return pltpu.make_async_copy(out.at[:, pl.ds(c0, w)], out_hbm.at[:, pl.ds(c0, w)], out_s.at[t])

    def l5_step(t, a, pb, rb, rb2, c0, w):
        u, v = coords(a)
        h = rows // 2
        near(rb2, w2, t)
        sym = s1_in[:, :, pl.ds(c0, w)].reshape(rows, w) + ps_in[:, pl.ds(c0, w)]
        out[:h, pl.ds(c0, w)] = pb[u, v, :h] + rb2[4] + rb2[3] + sym[:h]
        out[h:, pl.ds(c0, w)] = pb[u, v, h:] + rb2[2] + rb2[5] + sym[h:]
        o_copy(t, c0, w).start()

    def at(t):
        return (t, 1 - t % 2, p_b.at[t], r1.at[t], r2.at[t])

    def col0(t):
        return pl.multiple_of((t // 2) * CW + (t % 2) * (N_CH // 2) * CW, LANE)

    def loop(lo, fn, hi=N_CH):
        lax.fori_loop(lo, hi, lambda t, c: (fn(t), c)[1], 0)

    tail = (N_CH, 1, p_t, r1t, r2t)
    ct = N_CH * CW

    def run1(t):
        n, a, pb, rb, _ = at(t)
        l1_step(n, a, pb, rb, col0(t), CW)

    def run2(t):
        add_step(True, *at(t)[:4])

    def run3(t):
        l3_step(*at(t))

    def run4(t):
        n, a, pb, _, rb2 = at(t)
        add_step(False, n, a, pb, rb2)

    loop(0, run1, EARLY)
    b_fwd = onward(b0, b1, b2, b3)
    loop(EARLY, run1)
    l1_step(*tail[:4], ct, TAIL)
    loop(0, lambda t: plain_step(*at(t)[:4]))
    plain_step(*tail[:4])
    r3_work(a_fwd)
    loop(0, run2)
    add_step(True, *tail[:4])
    r5_work(b_fwd)
    loop(0, run3, EARLY + 1)
    ps_ready()
    ps_send(1, ROWS)
    loop(EARLY + 1, run3)
    l3_step(*tail)
    loop(0, run4, EARLY + 1)
    loop(EARLY + 1, run4)
    add_step(False, *tail[:3], r2t)
    s_own[0].wait()
    ps_own.wait()
    for k in range(1, RING):
        s_copy(0, k).wait_recv()
    for k in range(1, ROWS):
        ps_copy(k).wait_recv()
    l5_step(*tail, ct, TAIL)
    loop(0, lambda t: l5_step(*at(t), col0(t), CW))
    for i in range(N_CH + 1):
        o_copy(i, i * CW, CW if i < N_CH else TAIL).wait()

    for sem, bufs in ((s1, (r1, r1t)), (s2, (r2, r2t))):
        for i in range(2):
            pltpu.make_async_copy(bufs[i], bufs[i], sem.at[i]).wait()
    for c in (g0, g1, g2, g3, a0, a1, b0, b1, *a_fwd, *b_fwd):
        c.wait_send()
    pltpu.make_async_copy(t_others, t_others, t_s).wait()
    for k in range(1, RING):
        h_copy(k).wait_send()
    pltpu.make_async_copy(others, others, x_s).wait()
    for k in range(1, RING):
        m_copy(k).wait_send()
        s_copy(0, k).wait_send()
        s_copy(1, k).wait_send()
    for k in range(1, ROWS):
        ps_copy(k).wait_send()


def sweep_call(t_blk, oovv, wd, wx, v, oo):
    rows, cols = t_blk.shape
    n_c = v.shape[0]
    n_p = cols // n_c
    n_k, n_v, n_j = wd.shape
    k8 = rows // RING
    n_i = PLANE * rows
    blk = (RING, k8, cols)
    n = N_CH + 1
    pad1 = 48
    tv_shape = (RING, n_p, 2, k8, n_c)
    l1_shape, l2_shape = (pad1, n_k * n_v), (n_v, n_k * (FULL + EDGE))
    dma = pltpu.SemaphoreType.DMA
    vm = pl.BlockSpec(memory_space=pltpu.VMEM)
    hbm = pl.BlockSpec(memory_space=pl.ANY)

    def b16(*shape):
        return pltpu.VMEM(shape, BF16)

    def f32(*shape):
        return pltpu.VMEM(shape, F32)

    def sems(*shape):
        return dma(shape)

    one, two, four, six = (), (2,), (RING,), (n, 3)
    v9 = (-(-cols // 640),)
    counts = [four, four, four, four, one, one, four, four, four, four, one, one, (8,), two, two, two,
              v9, v9, v9, one, one, one, one, four, four, two, six, two, six, (2, RING), (2, RING), (ROWS,), (ROWS,), (n,), two]
    return pl.pallas_call(
        sweep_kernel,
        out_shape=jax.ShapeDtypeStruct((rows, cols), F32),
        in_specs=[vm, vm, hbm, hbm, hbm, hbm],
        out_specs=hbm,
        scratch_shapes=[
            b16(*tv_shape), b16(*l1_shape), b16(*l2_shape), b16(rows, cols),
            b16(*tv_shape), b16(2, 2, PLANE, k8, n_c), b16(2, PLANE, k8, n_c), b16(RING, 2, PLANE, k8, n_c),
            b16(RING, *l1_shape), b16(RING, *l2_shape),
            b16(2, RING, n_v, n_j), b16(2, n_k // 2, FULL, n_j), b16(2, n_k, EDGE, n_j),
            f32(n_v, n_j), f32(n_v, n_j), f32(k8, n_v, n_v), f32(k8, n_v, n_v), f32(2, *blk), f32(*blk), f32(*blk), f32(rows, cols), f32(rows, cols), b16(2, k8, 2 * n_i), f32(2, k8, n_i),
            b16(2, n_c, cols), b16(2, rows, cols), b16(n_i, 2 * rows),
            f32(2, PLANE, k8, n_i), f32(PLANE, 2, k8, n_i), b16(RING, 2, k8, n_i),
            f32(N_CH, RING, RING, rows, CW), f32(RING, RING, rows, TAIL),
            f32(N_CH, 6, 2, rows, CW), f32(6, 2, rows, TAIL),
            f32(N_CH, 6, rows // 2, CW), f32(6, rows // 2, TAIL),
        ] + [sems(*c) if c else dma for c in counts],
        compiler_params=pltpu.CompilerParams(has_side_effects=True, collective_id=0, vmem_limit_bytes=VMEM_LIMIT),
        name="sweep",
    )(t_blk, oovv, wd, wx, v, oo)


def solution(mesh):
    n_col = mesh.shape["col"]
    amp_spec = P("row", "col")
    wide_spec = P(None, "col")

    def local_sweep(t_blk, d_blk, oovv_blk, vvvv_blk, oooo_full, wd_blk, wx_blk):
        rows_dev, cols_dev = t_blk.shape
        n_occ = math.isqrt(oooo_full.shape[0])
        n_virt = wd_blk.shape[0] // n_occ
        occ_col = n_occ // n_col
        wd3 = wd_blk.reshape(n_occ, n_virt, occ_col * n_virt)
        wx3 = wx_blk.reshape(n_occ, n_virt, occ_col * n_virt)
        summed = sweep_call(t_blk, oovv_blk, wd3, wx3, vvvv_blk, oooo_full)
        return (oovv_blk.astype(F32) + summed) / d_blk

    return jax.shard_map(local_sweep, mesh=mesh, in_specs=(amp_spec, amp_spec, amp_spec, amp_spec, P(), wide_spec, wide_spec), out_specs=amp_spec, check_vma=False)
```

```python
import math
import jax
import jax.numpy as jnp
from jax import lax
from jax.experimental import pallas as pl
from jax.experimental.pallas import tpu as pltpu
from jax.sharding import PartitionSpec as P

MESH = pl.DeviceIdType.MESH
BF16 = jnp.bfloat16
F32 = jnp.float32
VMEM_LIMIT = 67_043_328
LANE = 128
RING = 4
PLANE = 16
ROWS = 32
FULL = 32
EDGE = 8
N_CH = 10
EARLY = 5
CW = 512
TAIL = 64


def _place():
    x = lax.axis_index("col")
    r = lax.axis_index("row")
    q = r // 2
    return x, q // RING, q % RING, r % 2, q, r


def _rc(src, dst, ssem, rsem, dev):
    return pltpu.make_async_remote_copy(src_ref=src, dst_ref=dst, send_sem=ssem, recv_sem=rsem, device_id=dev, device_id_type=MESH)


def _enter(x, r):
    bar = pltpu.get_barrier_semaphore()

    def tell(dev):
        pl.semaphore_signal(bar, inc=1, device_id=dev, device_id_type=MESH)

    for k in range(1, RING):
        tell(((x + k) % RING, r))
    for k in range(1, ROWS):
        tell((x, (r + k) % ROWS))

    pl.semaphore_wait(bar, RING - 1 + ROWS - 1)


def sweep_kernel(t_in, ov_in, d_in, wd, wx, v_hbm, oo_hbm, out_hbm,
                 tv, l1, l2, t2,
                 h_in, hv, vo, tl, lg1, lg2, wdb, wxb, wxs, d_n, e_n, s_f, s_b, sw, s1_in, s2_in, ps_in, out, oo2, oo, v_buf, t_pair, m_t, x_part, x_in, m_all,
                 p_b, p_t, r1, r1t, r2, r2t,
                 g_s, g_r, h_s, h_r, t_s, t_r, p_s, p_r, o_s, o_r, f_s, f_r, loc, wd_s, wx_s, wy_s,
                 vl_s, vx_s, vx_r, tp_s, tp_r, x_s, x_r, m_s, m_r, s1, w1, s2, w2, sw_s, sw_r, ps_s, ps_r, out_s, oo_s):
    x, z, y, core, q, r = _place()
    right, left = (x + 1) % RING, (x + RING - 1) % RING
    mate = (x, q * 2 + 1 - core)
    n_kd, n_v, n_j = wd.shape
    k8, n_c = tl.shape[3:]
    rows = RING * k8
    loc_g, loc_t, loc_1, loc_2, loc_v, loc_p, loc_a, loc_b = [loc.at[i] for i in range(loc.shape[0])]

    t2[...] = t_in[...].astype(BF16)
    for xd in range(RING):
        rq = slice(xd * k8, (xd + 1) * k8)
        for i, val in enumerate((t_in[rq, :], ov_in[rq, :].astype(F32))):
            for p in range(tv.shape[1]):
                tv[xd, p, i] = val[:, p * n_c:(p + 1) * n_c].astype(BF16)
    _enter(x, r)

    def ring(src, buf, ss, rr, axis):
        h = src.shape[axis] // 2

        def part(i):
            return (pl.ds(i * h, h),) if axis == 0 else (slice(None), pl.ds(i * h, h))

        def hop(i, who, blk, to):
            ref = buf.at[(blk,) + part(i - 2)]
            return _rc(ref, ref, ss.at[i], rr.at[i], (to, who))

        c0 = _rc(src, buf.at[x], ss.at[0], rr.at[0], (right, r))
        c1 = _rc(src, buf.at[x], ss.at[1], rr.at[1], (left, r))
        return c0, c1, lambda: hop(2, r, left, right), lambda: hop(3, r, right, left)

    own1 = pltpu.make_async_copy(l1, lg1.at[x], loc_1)
    own2 = pltpu.make_async_copy(l2, lg2.at[x], loc_2)
    def h_copy(k):
        xd = (x + k) % RING
        return _rc(tv.at[xd], h_in.at[x], h_s.at[k], h_r.at[k], (xd, r))

    for k in (1, RING - 1, 2):
        h_copy(k).start()

    def onward(r0, r1_, f0, f1):
        r0.wait_recv()
        f0 = f0()
        f0.start()
        r1_.wait_recv()
        f1 = f1()
        f1.start()
        return [f0, f1]

    def wd_copy(i):
        return pltpu.make_async_copy(wd.at[pl.ds(RING * i, RING)], wdb.at[i % 2], wd_s.at[i % 2])

    def wx_copy(i):
        c, h = i // 2, n_kd // 2
        src = wx.at[pl.ds(i % 2 * h, h), pl.ds(FULL * c + EDGE * ((c + 1) // 2), FULL)]
        return pltpu.make_async_copy(src, wxb.at[i % 2], wx_s.at[i % 2])

    def wy_copy(i):
        return pltpu.make_async_copy(wx.at[:, pl.ds(FULL + n_v // 2 * i, EDGE)], wxs.at[i], wy_s.at[i])

    def oo_copy(i):
        k0 = pl.multiple_of((2 * q + i) * rows + x * EDGE, EDGE)
        return pltpu.make_async_copy(oo_hbm.at[pl.ds(k0, EDGE)], oo2.at[i], oo_s.at[i])

    for i in range(2):
        oo_copy(i).start()
        wd_copy(i).start()
        wx_copy(i).start()
        wy_copy(i).start()

    def piece(xs, yd, buf):
        return buf.at[xs, pl.ds(2 * yd, 2)]

    def t_copy(xs, yd, buf):
        return _rc(piece(xs, yd, buf), hv.at[:, :, q], t_s, t_r, (x, (xs * RING + yd) * 2 + core))

    def t_own(xs, buf):
        return pltpu.make_async_copy(piece(xs, y, buf), hv.at[:, :, q], loc_t)

    def t_block(rel):
        xs = (x + rel) % RING
        buf = tv if rel == 0 else h_in
        for k in range(RING):
            yd = (y + k) % RING
            if k == 0:
                pl.when(xs == z)(lambda: t_own(xs, buf).start())
                pl.when(xs != z)(lambda: t_copy(xs, yd, buf).start())
            else:
                t_copy(xs, yd, buf).start()

    t_block(0)
    quarter = n_v // RING
    groups = t2.shape[0] // EDGE
    for a in range(quarter):
        for kk in range(groups):
            s_f[:, quarter * kk + a, :] = t_in[EDGE * kk:EDGE * (kk + 1), n_v * a:n_v * (a + 1)]
    rest = quarter - FULL
    odd = x % 2 == 1
    none = jnp.zeros((n_v, EDGE - rest), F32)
    for k in range(t2.shape[0]):
        kk = k // EDGE
        bt = s_f[k % EDGE, quarter * kk:quarter * (kk + 1), :].T
        e_n[:, FULL * k:FULL * (k + 1)] = jnp.where(odd, bt[:, rest:], bt[:, :FULL])
        d_n[:, EDGE * k:EDGE * (k + 1)] = jnp.where(odd, jnp.concatenate([none, bt[:, :rest]], axis=1), jnp.concatenate([bt[:, FULL:], none], axis=1))
    l2[:, :FULL * n_kd] = e_n[:, :FULL * n_kd].astype(BF16)
    l2[:, FULL * n_kd:] = d_n[:, :EDGE * n_kd].astype(BF16)
    pad1 = l1.shape[0]
    d_n[:pad1, :] = jnp.zeros((pad1, n_j), F32)
    for kk in range(groups):
        for i in range(EDGE):
            d_n[:quarter, n_v * i:n_v * (i + 1)] = s_f[i, quarter * kk:quarter * (kk + 1), :]
        l1[:, n_j * kk:n_j * (kk + 1)] = d_n[:pad1, :].astype(BF16)
    own1.start()
    own2.start()
    a0, a1, a2, a3 = ring(l1, lg1, p_s, p_r, 1)
    b0, b1, b2, b3 = ring(l2, lg2, o_s, o_r, 1)
    a0.start()
    a1.start()
    for k in (1, RING - 1, 2):
        h_copy(k).wait_recv()
        t_block(RING - k)

    n_v9 = vl_s.shape[0]
    wide = 640
    v_in = []
    for i in range(n_v9):
        c0 = i * wide
        w = min(wide, v_hbm.shape[1] - c0)
        src, dst = v_hbm.at[:, pl.ds(c0, w)], v_buf.at[core, :, pl.ds(c0, w)]
        v_in += [pltpu.make_async_copy(src, dst, vl_s.at[i]), _rc(src, dst, vx_s.at[i], vx_r.at[i], mate)]
    v_in += [pltpu.make_async_copy(t2, t_pair.at[core], loc_p), _rc(t2, t_pair.at[core], tp_s, tp_r, mate)]
    for c in v_in:
        c.start()

    for i in range(2):
        oo_copy(i).wait()
    ow = oo2[...].astype(F32)
    for k in range(PLANE):
        c0 = 2 * k * rows
        oo[:, :, k * rows:(k + 1) * rows] = jnp.where(core == 1, ow[:, :, c0 + rows:c0 + 2 * rows], ow[:, :, c0:c0 + rows])
    ot = oo[...].reshape(2 * k8, PLANE * rows).T
    ot = jnp.concatenate([ot[k * rows + i * k8:k * rows + (i + 1) * k8] for i in range(RING) for k in range(PLANE)], axis=0)
    oo[...] = ot.T.reshape(2, k8, PLANE * rows)

    t_own(x, tv).wait()
    t_others = hv.at[:, :, pl.ds(0, PLANE - 1)]
    pltpu.make_async_copy(t_others, t_others, t_r).wait()
    g0, g1, g2, g3 = ring(hv.at[:, 0], tl, g_s, g_r, 0)
    g0.start()
    g1.start()
    fwd = _rc(hv.at[:, 1], vo, f_s, f_r, mate)
    fwd.start()
    own = pltpu.make_async_copy(hv.at[:, 0], tl.at[x], loc_g)
    own.start()
    g0.wait_recv()
    g2 = g2()
    g2.start()
    g1.wait_recv()
    g3 = g3()
    g3.start()
    a_fwd = onward(a0, a1, a2, a3)
    fwd.wait()
    own.wait()
    g2.wait_recv()
    g3.wait_recv()

    n_i = PLANE * rows
    n_k = PLANE * k8
    dn = (((1,), (1,)), ((), ()))

    def x_of(v_mine, v_ref):
        acc = None
        for i in range(2):
            v_i = (v_ref[i, 1] if v_mine else v_ref[i]).reshape(n_k, n_c)
            d = lax.dot_general(v_i, tl[:, i].reshape(n_i, n_c), dn, preferred_element_type=F32)
            acc = d if acc is None else acc + d
        return acc.reshape(PLANE, k8, n_i)

    x_part[core] = x_of(True, hv)
    x_part[1 - core] = x_of(False, vo)

    def x_copy(k):
        qd = (q + k) % PLANE
        return _rc(x_part.at[:, qd], x_in.at[q], x_s, x_r, (x, qd * 2 + core))

    for k in range(1, PLANE):
        x_copy(k).start()
    x_in[q] = x_part[:, q]
    others = x_in.at[pl.ds(0, PLANE - 1)]
    pltpu.make_async_copy(others, others, x_r).wait()
    xs = x_in[0]
    for k in range(1, PLANE):
        xs = xs + x_in[k]
    m_all[x] = (oo[...] + 0.5 * xs).astype(BF16)

    def m_copy(k):
        return _rc(m_all.at[x], m_all.at[x], m_s.at[k], m_r.at[k], ((x + k) % RING, r))

    for k in range(1, RING):
        m_copy(k).start()
    b0.start()
    b1.start()

    def s_copy(i, k):
        xd = (x + k) % RING
        return _rc(sw.at[i, xd], (s1_in, s2_in)[i].at[x], sw_s.at[i, k], sw_r.at[i, k], (xd, r))

    s_own = [pltpu.make_async_copy(sw.at[i, x], (s1_in, s2_in)[i].at[x], (loc_a, loc_b)[i]) for i in range(2)]
    def ps_src(rd):
        return s2_in.at[rd // EDGE, pl.ds(rd % EDGE, 1)]

    def ps_copy(k):
        rd = (r + k) % ROWS
        return _rc(ps_src(rd), ps_in.at[pl.ds(r, 1)], ps_s.at[k], ps_r.at[k], (x, rd))

    ps_own = pltpu.make_async_copy(ps_src(r), ps_in.at[pl.ds(r, 1)], loc_g)

    def ps_ready():
        s_own[1].wait()
        for k in range(1, RING):
            s_copy(1, k).wait_recv()
        ps_own.start()

    def ps_send(lo, hi):
        for k in range(lo, hi):
            ps_copy(k).start()

    n1 = l1.shape[0]

    def r3_work(a_fwd):
        own1.wait()
        own2.wait()
        for c in a_fwd:
            c.wait_recv()
        acc = None
        kd = RING * n_v
        for i in range(2 * RING):
            wd_copy(i).wait()
            lhs = lg1[:, :, i * kd:(i + 1) * kd].reshape(RING * n1, kd)
            d = jnp.dot(lhs, wdb[i % 2].reshape(kd, n_j), preferred_element_type=F32)
            acc = d if acc is None else acc + d
            if i + 2 < 2 * RING:
                wd_copy(i + 2).start()
        for i in range(RING):
            d_n[quarter * i:quarter * (i + 1), :] = acc[n1 * i:n1 * i + quarter]

    def r5_work(b_fwd):
        for c in b_fwd:
            c.wait_recv()
        acc = None
        kb = FULL * n_kd
        kh = kb // 2
        for i in range(2 * RING):
            wx_copy(i).wait()
            d = jnp.dot(lg2[i // 2, :, i % 2 * kh:(i % 2 + 1) * kh], wxb[i % 2].reshape(kh, n_j), preferred_element_type=F32)
            acc = d if acc is None else acc + d
            if i + 2 < 2 * RING:
                wx_copy(i + 2).start()
        for i in range(2):
            wy_copy(i).wait()
            lhs = lg2[2 * i, :, kb:] + lg2[2 * i + 1, :, kb:]
            acc = acc + jnp.dot(lhs, wxs[i].reshape(EDGE * n_kd, n_j), preferred_element_type=F32)
        e_n[...] = acc

        for j in range(n_j // n_v):
            cut = slice(j * n_v, (j + 1) * n_v)
            sj = d_n[:, cut] - e_n[:, cut].T
            s_f[j] = sj
            s_b[j] = sj.T
        for i in range(2):
            for a in range(n_v):
                c0 = a % quarter * n_v
                sw[i, a // quarter, :, c0:c0 + n_v] = (s_f, s_b)[i][:, a, :]
        for i in (1, 0):
            for k in range(1, RING):
                s_copy(i, k).start()
            s_own[i].start()


    for c in v_in:
        c.wait()
    for k in range(1, RING):
        m_copy(k).wait_recv()
    mf = m_all[...].astype(F32)
    m_t[...] = jnp.concatenate([mf[xx, cc] for cc in range(2) for xx in range(RING)], axis=0).T.astype(BF16)

    def to(first, a, d):
        b = a if first else 1 - a
        return (x, (((z + d * (1 - b)) % RING) * RING + (y + d * b) % RING) * 2 + core)

    def coords(a):
        return y * a + z * (1 - a), z * a + y * (1 - a)

    def stage(first, t, a, pb, rb):
        u, v = coords(a)
        c, pre, n = (u, (), 2) if first else (v, (u,), rows // 2)
        lo, hi = pl.ds(0, n), pl.ds(n, n)
        far, up, dn_ = (c + 2) % RING, (c + 1) % RING, (c + RING - 1) % RING
        ss, ww = (s1, w1) if first else (s2, w2)
        last = isinstance(t, int) and t == N_CH
        srcs = (far, lo), (far, hi), (up, hi), (dn_, lo), (up, lo), (dn_, hi)

        def msg(i):
            d = 1 if i % 2 == 0 else RING - 1
            return _rc(pb.at[pre + srcs[i]], rb.at[i], ss.at[int(last)], ww.at[t, min(i, 2)], to(first, a, d))
        return msg

    def near(rb, ww, t):
        got = rb.at[pl.ds(2, 4)]
        pltpu.make_async_copy(got, got, ww.at[t, 2]).wait()

    def l1_step(t, a, pb, rb, c0, w):
        tp = t_pair[:, :, pl.ds(c0, w)].reshape(2 * rows, w)
        acc = jnp.dot(m_t[...], tp, preferred_element_type=F32)
        for i in range(2):
            acc = acc + jnp.dot(tl[:, i].reshape(n_i, n_c), v_buf[i, :, pl.ds(c0, w)], preferred_element_type=F32)
        for zb in range(RING):
            for yb in range(RING):
                for i in range(RING):
                    b = i * n_k + (zb * RING + yb) * k8
                    pb[yb * a + zb * (1 - a), zb * a + yb * (1 - a), i * k8:(i + 1) * k8] = acc[b:b + k8]
        msg = stage(True, t, a, pb, rb)
        msg(0).start()
        msg(1).start()

    def plain_step(t, a, pb, rb):
        msg = stage(True, t, a, pb, rb)
        msg(2).start()
        msg(3).start()

    def add_step(first, t, a, pb, rb):
        u, v = coords(a)
        c, pre, n = (u, (), 2) if first else (v, (u,), rows // 2)
        msg = stage(first, t, a, pb, rb)
        msg(0).wait_recv()
        up = pre + ((c + 1) % RING, pl.ds(0, n))
        pb[up] = pb[up] + rb[0]
        msg(4).start()
        msg(1).wait_recv()
        dn_ = pre + ((c + RING - 1) % RING, pl.ds(n, n))
        pb[dn_] = pb[dn_] + rb[1]
        msg(5).start()

    def l3_step(t, a, pb, rb, rb2):
        u, _ = coords(a)
        near(rb, w1, t)
        pb[u, :2] = pb[u, :2] + rb[4] + rb[3]
        pb[u, 2:] = pb[u, 2:] + rb[2] + rb[5]
        nxt = stage(False, t, a, pb, rb2)
        for i in range(4):
            nxt(i).start()

    def o_copy(t, c0, w):
        return pltpu.make_async_copy(out.at[:, pl.ds(c0, w)], out_hbm.at[:, pl.ds(c0, w)], out_s.at[t])

    def l5_step(t, a, pb, rb, rb2, c0, w):
        u, v = coords(a)
        h = rows // 2
        near(rb2, w2, t)
        sym = s1_in[:, :, pl.ds(c0, w)].reshape(rows, w) + ps_in[:, pl.ds(c0, w)]
        sym = sym + ov_in[:, pl.ds(c0, w)].astype(F32)
        out[:h, pl.ds(c0, w)] = (pb[u, v, :h] + rb2[4] + rb2[3] + sym[:h]) / d_in[:h, pl.ds(c0, w)]
        out[h:, pl.ds(c0, w)] = (pb[u, v, h:] + rb2[2] + rb2[5] + sym[h:]) / d_in[h:, pl.ds(c0, w)]
        o_copy(t, c0, w).start()

    def at(t):
        return (t, 1 - t % 2, p_b.at[t], r1.at[t], r2.at[t])

    def col0(t):
        return pl.multiple_of((t // 2) * CW + (t % 2) * (N_CH // 2) * CW, LANE)

    def loop(lo, fn, hi=N_CH):
        lax.fori_loop(lo, hi, lambda t, c: (fn(t), c)[1], 0)

    tail = (N_CH, 1, p_t, r1t, r2t)
    ct = N_CH * CW

    def run1(t):
        n, a, pb, rb, _ = at(t)
        l1_step(n, a, pb, rb, col0(t), CW)

    def run2(t):
        add_step(True, *at(t)[:4])

    def run3(t):
        l3_step(*at(t))

    def run4(t):
        n, a, pb, _, rb2 = at(t)
        add_step(False, n, a, pb, rb2)

    loop(0, run1, EARLY)
    b_fwd = onward(b0, b1, b2, b3)
    loop(EARLY, run1)
    l1_step(*tail[:4], ct, TAIL)
    loop(0, lambda t: plain_step(*at(t)[:4]))
    plain_step(*tail[:4])
    r3_work(a_fwd)
    loop(0, run2)
    add_step(True, *tail[:4])
    r5_work(b_fwd)
    loop(0, run3, EARLY + 1)
    ps_ready()
    ps_send(1, ROWS)
    loop(EARLY + 1, run3)
    l3_step(*tail)
    loop(0, run4, EARLY + 1)
    loop(EARLY + 1, run4)
    add_step(False, *tail[:3], r2t)
    s_own[0].wait()
    ps_own.wait()
    for k in range(1, RING):
        s_copy(0, k).wait_recv()
    for k in range(1, ROWS):
        ps_copy(k).wait_recv()
    l5_step(*tail, ct, TAIL)
    loop(0, lambda t: l5_step(*at(t), col0(t), CW))
    for i in range(N_CH + 1):
        o_copy(i, i * CW, CW if i < N_CH else TAIL).wait()

    for sem, bufs in ((s1, (r1, r1t)), (s2, (r2, r2t))):
        for i in range(2):
            pltpu.make_async_copy(bufs[i], bufs[i], sem.at[i]).wait()
    for c in (g0, g1, g2, g3, a0, a1, b0, b1, *a_fwd, *b_fwd):
        c.wait_send()
    pltpu.make_async_copy(t_others, t_others, t_s).wait()
    for k in range(1, RING):
        h_copy(k).wait_send()
    pltpu.make_async_copy(others, others, x_s).wait()
    for k in range(1, RING):
        m_copy(k).wait_send()
        s_copy(0, k).wait_send()
        s_copy(1, k).wait_send()
    for k in range(1, ROWS):
        ps_copy(k).wait_send()


def sweep_call(t_blk, oovv, den, wd, wx, v, oo):
    rows, cols = t_blk.shape
    n_c = v.shape[0]
    n_p = cols // n_c
    n_k, n_v, n_j = wd.shape
    k8 = rows // RING
    n_i = PLANE * rows
    blk = (RING, k8, cols)
    n = N_CH + 1
    pad1 = 48
    tv_shape = (RING, n_p, 2, k8, n_c)
    l1_shape, l2_shape = (pad1, n_k * n_v), (n_v, n_k * (FULL + EDGE))
    dma = pltpu.SemaphoreType.DMA
    vm = pl.BlockSpec(memory_space=pltpu.VMEM)
    hbm = pl.BlockSpec(memory_space=pl.ANY)

    def b16(*shape):
        return pltpu.VMEM(shape, BF16)

    def f32(*shape):
        return pltpu.VMEM(shape, F32)

    def sems(*shape):
        return dma(shape)

    one, two, four, six = (), (2,), (RING,), (n, 3)
    v9 = (-(-cols // 640),)
    counts = [four, four, four, four, one, one, four, four, four, four, one, one, (8,), two, two, two,
              v9, v9, v9, one, one, one, one, four, four, two, six, two, six, (2, RING), (2, RING), (ROWS,), (ROWS,), (n,), two]
    return pl.pallas_call(
        sweep_kernel,
        out_shape=jax.ShapeDtypeStruct((rows, cols), F32),
        in_specs=[vm, vm, vm, hbm, hbm, hbm, hbm],
        out_specs=hbm,
        scratch_shapes=[
            b16(*tv_shape), b16(*l1_shape), b16(*l2_shape), b16(rows, cols),
            b16(*tv_shape), b16(2, 2, PLANE, k8, n_c), b16(2, PLANE, k8, n_c), b16(RING, 2, PLANE, k8, n_c),
            b16(RING, *l1_shape), b16(RING, *l2_shape),
            b16(2, RING, n_v, n_j), b16(2, n_k // 2, FULL, n_j), b16(2, n_k, EDGE, n_j),
            f32(n_v, n_j), f32(n_v, n_j), f32(k8, n_v, n_v), f32(k8, n_v, n_v), f32(2, *blk), f32(*blk), f32(*blk), f32(rows, cols), f32(rows, cols), b16(2, k8, 2 * n_i), f32(2, k8, n_i),
            b16(2, n_c, cols), b16(2, rows, cols), b16(n_i, 2 * rows),
            f32(2, PLANE, k8, n_i), f32(PLANE, 2, k8, n_i), b16(RING, 2, k8, n_i),
            f32(N_CH, RING, RING, rows, CW), f32(RING, RING, rows, TAIL),
            f32(N_CH, 6, 2, rows, CW), f32(6, 2, rows, TAIL),
            f32(N_CH, 6, rows // 2, CW), f32(6, rows // 2, TAIL),
        ] + [sems(*c) if c else dma for c in counts],
        compiler_params=pltpu.CompilerParams(has_side_effects=True, collective_id=0, vmem_limit_bytes=VMEM_LIMIT),
        name="sweep",
    )(t_blk, oovv, den, wd, wx, v, oo)


def solution(mesh):
    n_col = mesh.shape["col"]
    amp_spec = P("row", "col")
    wide_spec = P(None, "col")

    def local_sweep(t_blk, d_blk, oovv_blk, vvvv_blk, oooo_full, wd_blk, wx_blk):
        rows_dev, cols_dev = t_blk.shape
        n_occ = math.isqrt(oooo_full.shape[0])
        n_virt = wd_blk.shape[0] // n_occ
        occ_col = n_occ // n_col
        wd3 = wd_blk.reshape(n_occ, n_virt, occ_col * n_virt)
        wx3 = wx_blk.reshape(n_occ, n_virt, occ_col * n_virt)
        return sweep_call(t_blk, oovv_blk, d_blk, wd3, wx3, vvvv_blk, oooo_full)

    return jax.shard_map(local_sweep, mesh=mesh, in_specs=(amp_spec, amp_spec, amp_spec, amp_spec, P(), wide_spec, wide_spec), out_specs=amp_spec, check_vma=False)
```
